1024 devices in a mesh: ctx: 32 (over z, x_hi, core), tp: 32 (over x_lo, y).
Axes of the slice: x: 8 (x_hi: 2, x_lo: 4; x = x_hi * 4 + x_lo), y: 8, z: 8, core: 2. Of those that a mesh axis runs over, the one named last changes fastest.
Arguments:
- act_codes: bfloat16 [8192, 4096], P(('ctx', 'tp')), may hold values from -24 to 24
- scale_exps: int32 [8192, 32], P(('ctx', 'tp')), may hold values from -2 to 2
- weight: bfloat16 [4096, 6144], P(None, 'tp'), may hold values from -0.09375 to 0.09375
- grad_out: bfloat16 [8192, 6144], P('ctx', 'tp'), may hold values from -6 to 6
Outputs:
- grad_input: bfloat16 [8192, 4096], P(('ctx', 'tp'))
- grad_weight: float32 [4096, 6144], P('ctx', 'tp')
The draws below stay inside these ranges and needn't reach their ends.
All inputs are finite; a program needn't handle non-finite values.
Results may differ from the reference program's by a relative error of at most 0.023.
Values may be sent and summed in bfloat16 or wider, within the bound.
A program may use at most 32 MiB of HBM per device.

```python
import jax
import jax.numpy as jnp
from jax import lax

D = 4096
BLOCK = 128
QKVW = 6144
TOKENS = 8192
N_TP = 32


def plant(array, own_key, least, high):
    place = [jax.random.randint(jax.random.fold_in(own_key, axis), (), 0, length) for axis, length in enumerate(array.shape)]
    longest = array.shape.index(max(array.shape))
    neighbour = place[:longest] + [(place[longest] + 1) % array.shape[longest]] + place[longest + 1:]
    return array.at[tuple(place)].set(least).at[tuple(neighbour)].set(high)


def strengthened(array, own_key, source, target, parts, factor):
    owner, partner = [(jnp.arange(array.shape[axis_at]) // (array.shape[axis_at] // parts)).reshape([-1 if axis == axis_at else 1 for axis in range(array.ndim)]) for axis_at in (source, target)]
    chosen = jax.random.permutation(own_key, parts)[partner]
    strong = (owner == chosen) | (owner == (partner + parts // 2) % parts)
    return jnp.where(strong, factor * array, array)


def levels(stream_key, shape, shards, low, top_value):
    loudness, own = 1.0, jax.random.fold_in(stream_key, 6)
    for position, parts in shards:
        steps = jnp.exp(jax.random.uniform(jax.random.fold_in(own, position), (parts,), jnp.float32, low / len(shards), top_value / len(shards)))
        loudness = loudness * jnp.repeat(steps, shape[position] // parts).reshape([-1 if axis == position else 1 for axis in range(len(shape))])
    return loudness


def gaussian(own_key, dims, deviation, reach, cuts=(), kind=jnp.bfloat16):
    values = jax.random.normal(own_key, dims, jnp.float32) * deviation
    if len(cuts) > 0:
        values = levels(own_key, dims, cuts, -0.22, 0.18) * values
    return jnp.clip(values, min=-reach, max=reach).astype(kind)


def noise_with(stream_key, extent, scale, reach, pieces, heavy, held_as=jnp.bfloat16):
    drawn = scale * jax.random.normal(stream_key, extent, jnp.float32)
    if pieces:
        drawn = drawn * levels(stream_key, extent, pieces, -0.22, 0.18)
    return jnp.clip(strengthened(drawn, jax.random.fold_in(stream_key, 3), *heavy), -reach, reach).astype(held_as)


def setup_inputs(seed: int = 0) -> dict:
    key_list = jax.random.split(jax.random.key(seed), 5)
    act_codes = noise_with(key_list[0], (TOKENS, D), 1.0, 24.0, ((0, 1024),), (0, 1, 1024, 6.0))
    scale_exps = plant(jax.random.randint(key_list[1], (TOKENS, D // BLOCK), -2, 3), jax.random.fold_in(key_list[1], 1), -2, 2).astype(jnp.int32)
    weight = gaussian(key_list[2], (D, QKVW), D ** -0.5, 0.09375, ((1, 32),))
    grad_out = noise_with(key_list[3], (TOKENS, QKVW), 1.0, 6.0, ((0, 32), (1, 32)), (1, 0, 32, 2.75))
    return {"act_codes": act_codes, "scale_exps": scale_exps, "weight": weight, "grad_out": grad_out}


def dequantize(act_codes, scale_exps):
    tok_rows = act_codes.shape[0]
    scales = jnp.exp2(scale_exps.astype(jnp.float32))
    blocked = act_codes.astype(jnp.float32).reshape(tok_rows, D // BLOCK, BLOCK) * scales[:, :, None]
    return blocked.reshape(tok_rows, D).astype(jnp.bfloat16)

def reference(act_codes, scale_exps, weight, grad_out):
    acts = dequantize(act_codes, scale_exps)
    grad_weight = jnp.dot(acts.T, grad_out, preferred_element_type=jnp.float32)
    grad_weight = grad_weight * lax.rsqrt(jnp.float32(TOKENS))
    width = QKVW // N_TP

    def add_block(total, index):
        offset = (index * width).astype(jnp.int32)
        grads = lax.dynamic_slice_in_dim(grad_out, offset, width, 1)
        weights = lax.dynamic_slice_in_dim(weight, offset, width, 1)
        part = lax.dot_general(grads, weights, (((1,), (1,)), ((), ())), preferred_element_type=jnp.float32)
        part = lax.optimization_barrier(part.astype(jnp.bfloat16))
        return (total + part.astype(jnp.float32), None)
    total, unused = lax.scan(add_block, jnp.zeros((TOKENS, D), jnp.float32), jnp.arange(N_TP, dtype=jnp.int32))
    return (total.astype(jnp.bfloat16), grad_weight)
```

```python
import functools

import jax
import jax.numpy as jnp
from jax import lax
from jax.experimental import pallas as pl
from jax.experimental.pallas import tpu as pltpu
from jax.sharding import PartitionSpec as P

DIMS = {"z": 8, "xh": 2, "core": 2, "xl": 4, "y": 8}
GROUPS = 4


def ring_pieces(half, groups):
    low, high = tuple(range(groups // 2)), tuple(range(groups // 2, groups))
    ways = []
    for first, rest in ((low, high), (high, low)):
        order = [(1, g) for g in first]
        for step in range(2, half + 1):
            order += [(step, g) for g in rest + first]
        ways.append(order)
    return ways


def kernel(
    dims, scale, codes_hbm, exps_hbm, w_hbm, g_hbm, gi_ref, gw_ref,
    codes, exps, w, g, in_sem,
    s_buf, a1, ab, at, gp, ga, rest, parts, rb, xs, xr, own,
    dwf, dwb, rz, fs, fr,
    s_send, s_recv, a_send, a_recv, g_send, g_recv, p_send, p_recv,
    z_send, z_recv, x_send, x_recv, f_send, f_recv,
):
    nz, nh, nc, nx, ny = dims["z"], dims["xh"], dims["core"], dims["xl"], dims["y"]
    hy, hz = ny // 2, nz // 2
    f32, bf16 = jnp.float32, jnp.bfloat16
    ctx, tp = lax.axis_index("ctx"), lax.axis_index("tp")
    z, xh, c = ctx // (nh * nc), (ctx // nc) % nh, ctx % nc
    xl, y = tp // ny, tp % ny

    def at_z(d):
        return {"ctx": ((z + d + nz) % nz * nh + xh) * nc + c, "tp": tp}

    def at_y(d):
        return {"ctx": ctx, "tp": xl * ny + (y + d + ny) % ny}

    def at_x(dx, dc=0, dh=0):
        return {
            "ctx": (z * nh + (xh + dh) % nh) * nc + (c + dc) % nc,
            "tp": (xl + dx) % nx * ny + y,
        }

    rows, width = codes.shape
    toks, cols = g.shape
    blocks = exps.shape[1]
    quarter = 128 // nx
    feats = width // (nc * nx)
    per = rows * nx
    glanes = width // GROUPS
    sent = []

    def send(src, dst, ssem, rsem, dev):
        copy = pltpu.make_async_remote_copy(
            src_ref=src, dst_ref=dst, send_sem=ssem, recv_sem=rsem,
            device_id=dev, device_id_type=pl.DeviceIdType.MESH,
        )
        copy.start()
        sent.append(copy)
        return copy

    loads = []
    for i, (src, dst) in enumerate(((codes_hbm, codes), (exps_hbm, exps), (g_hbm, g), (w_hbm, w))):
        copy = pltpu.make_async_copy(src, dst, in_sem.at[i])
        copy.start()
        loads.append(copy)

    barrier = pltpu.get_barrier_semaphore()
    mates = [(dx, dc) for dx in range(nx) for dc in range(nc) if (dx, dc) != (0, 0)]
    finals = [(dh, dx) for dh in range(nh) for dx in range(nx) if (dh, dx) != (0, 0)]
    peers = [at_x(dx, dc) for dx, dc in mates]
    peers += [at_x(dx, 0, dh) for dh, dx in finals if dh != 0]
    peers += [at_y(1), at_y(-1), at_z(1), at_z(-1)]
    for dev in peers:
        pl.semaphore_signal(barrier, inc=1, device_id=dev, device_id_type=pl.DeviceIdType.MESH)

    loads[0].wait()
    loads[1].wait()
    scales = jnp.exp2(exps[...].astype(f32))
    lane = lax.broadcasted_iota(jnp.int32, (rows, 128), 1) // quarter
    acts = [
        codes[:, b * 128 : (b + 1) * 128].astype(f32) * scales[:, b : b + 1] for b in range(blocks)
    ]
    for xi in range(nx):
        for ci in range(nc):
            mine = [acts[b] for b in range(blocks) if b % nc == ci]
            for m in range(len(mine) // nx):
                out = mine[m * nx]
                if xi:
                    out = pltpu.roll(out, (128 - xi * quarter) % 128, 1)
                for i in range(1, nx):
                    piece, shift = mine[m * nx + i], ((i - xi) * quarter) % 128
                    if shift:
                        piece = pltpu.roll(piece, shift, 1)
                    out = jnp.where(lane == i, piece, out)
                s_buf[xi * nc + ci, :, m * 128 : (m + 1) * 128] = out.astype(bf16)
    a1[xl * nc + c] = s_buf[xl * nc + c]

    loads[2].wait()
    raw = g[...].astype(f32)
    raw = jnp.concatenate(
        [
            raw[(i * ny + j) * rows : (i * ny + j + 1) * rows]
            for j in range(ny) for i in range(nx)
        ],
        axis=0,
    )
    gp[...] = raw.astype(bf16)
    ga[c, xl, :toks, :] = raw[:, :128].astype(bf16)
    tail = raw[:, 128:]
    ga[c, xl, toks:, :] = jnp.concatenate([tail[: toks // 2], tail[toks // 2 :]], axis=1).astype(bf16)

    pl.semaphore_wait(barrier, len(peers))

    s_wait = []
    for k, (dx, dc) in enumerate(mates):
        s_wait.append(
            send(
                s_buf.at[(xl + dx) % nx * nc + (c + dc) % nc], a1.at[xl * nc + c],
                s_send.at[k], s_recv.at[k], at_x(dx, dc),
            )
        )
    g_wait = []
    for dx in range(1, nx):
        g_wait.append(
            send(ga.at[c, xl], ga.at[c, xl], g_send.at[dx - 1], g_recv.at[dx - 1], at_x(dx))
        )
    twin_wait = [
        send(ga.at[c, xl], ga.at[c, xl], g_send.at[nx - 1], g_recv.at[nx - 1], at_x(0, 1))
    ]

    loads[3].wait()
    step_w = min(width, 512)
    for n in range(width // step_w):
        part = lax.dot_general(
            gp[...], w[n * step_w : (n + 1) * step_w, :], (((1,), (1,)), ((), ())),
            preferred_element_type=f32,
        )
        parts[:, :, n * step_w : (n + 1) * step_w] = part.astype(bf16).reshape(ny, per, step_w)

    p_orders = ring_pieces(hy, GROUPS)
    p_index = [{piece: i for i, piece in enumerate(order)} for order in p_orders]
    p_copies = [{}, {}]
    p_next = [0, 0]

    def p_piece(way):
        if p_next[way] >= len(p_orders[way]):
            return
        step, grp = p_orders[way][p_next[way]]
        p_next[way] += 1
        sign = 1 - 2 * way
        off = hy + 1 - step
        lanes = slice(grp * glanes, (grp + 1) * glanes)
        dest = (y + sign * off + ny) % ny
        if (step - 1, grp) in p_copies[way]:
            p_copies[way][(step - 1, grp)].wait_recv()
            total = rb[way, step - 2, :, lanes].astype(f32) + parts[dest, :, lanes].astype(f32)
            rb[way, step - 2, :, lanes] = total.astype(bf16)
            src = rb.at[way, step - 2, :, lanes]
        else:
            src = parts.at[dest, :, lanes]
        i = p_index[way][(step, grp)]
        p_copies[way][(step, grp)] = send(
            src, rb.at[way, step - 1, :, lanes], p_send.at[way, i], p_recv.at[way, i], at_y(sign)
        )

    def p_both(count=1):
        for _ in range(count):
            p_piece(0)
            p_piece(1)

    p_both(GROUPS // 2)

    for copy in s_wait:
        copy.wait_recv()
    for ci in range(nc):
        ab[y, ci] = jnp.concatenate(
            [a1[xi * nc + ci].astype(f32) for xi in range(nx)], axis=0
        ).astype(bf16)

    a_copies = [{}, {}]

    def a_piece(way, step, ci):
        sign = 1 - 2 * way
        if step > 1:
            a_copies[way][(step - 1, ci)].wait_recv()
        ref = ab.at[(y - sign * (step - 1) + ny) % ny, ci]
        i = (step - 1) * nc + ci
        a_copies[way][(step, ci)] = send(ref, ref, a_send.at[way, i], a_recv.at[way, i], at_y(sign))

    for step in range(1, hy + 1):
        for ci in range(nc):
            for way in (0, 1):
                if step < hy or ci % 2 == way:
                    a_piece(way, step, ci)
        p_both()

    for dx in range(1, nx):
        g_wait[dx - 1].wait_recv()
        ref = ga.at[c, (xl - dx + nx) % nx]
        twin_wait.append(
            send(ref, ref, g_send.at[nx - 1 + dx], g_recv.at[nx - 1 + dx], at_x(0, 1))
        )

    for way in (0, 1):
        for ci in range(nc):
            if (hy, ci) in a_copies[way]:
                a_copies[way][(hy, ci)].wait_recv()
            if hy > 1 and not (hy, ci) in a_copies[way]:
                a_copies[way][(hy - 1, ci)].wait_recv()
    for ci in range(nc):
        at[:, ci * toks : (ci + 1) * toks] = ab[:, ci].reshape(toks, feats).T
    for copy in twin_wait:
        copy.wait_recv()

    mains = nx * 128
    for ci in range(nc):
        for k in range(nx // 2):
            left = ga[ci, 2 * k, toks:, :].astype(f32)
            right = ga[ci, 2 * k + 1, toks:, :].astype(f32)
            first = lax.broadcasted_iota(jnp.int32, left.shape, 1) < 64
            top = jnp.where(first, left, pltpu.roll(right, 64, 1))
            bottom = jnp.where(first, pltpu.roll(left, 64, 1), right)
            lanes = slice(k * 128, (k + 1) * 128)
            rest[ci * toks : ci * toks + toks // 2, lanes] = top.astype(bf16)
            rest[ci * toks + toks // 2 : (ci + 1) * toks, lanes] = bottom.astype(bf16)
    zrows = feats // nz

    def dw_store(lanes, value):
        value = value.reshape(nz, zrows, value.shape[1])
        dwf[:, :, lanes] = value
        dwb[:, :, lanes] = value.astype(bf16)

    for k in range(nx // 2):
        total = None
        for ci in range(nc):
            both = jnp.concatenate([ga[ci, 2 * k, :toks, :], ga[ci, 2 * k + 1, :toks, :]], axis=1)
            part = jnp.dot(at[:, ci * toks : (ci + 1) * toks], both, preferred_element_type=f32)
            total = part if total is None else total + part
        dw_store(slice(k * 256, (k + 1) * 256), total)
    dw_store(slice(mains, mains + 64 * nx), jnp.dot(at[...], rest[...], preferred_element_type=f32))

    z_orders = ring_pieces(hz, 2)
    z_copies = [{}, {}]
    half_rows = zrows // 2

    def z_total(way, step, grp, dest):
        z_copies[way][(step, grp)].wait_recv()
        sub = slice(grp * half_rows, (grp + 1) * half_rows)
        return rz[way, step - 1, sub, :].astype(f32)

    def z_piece(way, i):
        step, grp = z_orders[way][i]
        sign = 1 - 2 * way
        dest = (z + sign * (hz + 1 - step) + nz) % nz
        sub = slice(grp * half_rows, (grp + 1) * half_rows)
        if (step - 1, grp) in z_copies[way]:
            total = z_total(way, step - 1, grp, dest) + dwf[dest, sub, :]
            rz[way, step - 2, sub, :] = total.astype(bf16)
            src = rz.at[way, step - 2, sub, :]
        else:
            src = dwb.at[dest, sub, :]
        z_copies[way][(step, grp)] = send(
            src, rz.at[way, step - 1, sub, :], z_send.at[way, i], z_recv.at[way, i], at_z(sign)
        )

    for i in range(len(z_orders[0])):
        z_piece(0, i)
        z_piece(1, i)
        p_both()

    f_wait = []
    sums = []
    for grp in range(2):
        sub = slice(grp * half_rows, (grp + 1) * half_rows)
        total = dwf[z, sub, :]
        for way in (0, 1):
            if (hz, grp) in z_copies[way]:
                total = total + z_total(way, hz, grp, z)
        sums.append(total)
    frows = zrows // nh
    total = sums if nh == 2 else [jnp.concatenate(sums, axis=0)]
    for hi in range(nh):
        for xi in range(nx):
            fs[hi, xi, :, :128] = total[hi][:, xi * 128 : (xi + 1) * 128].astype(bf16)
            lo = mains + xi // 2 * 128
            fs[hi, xi, :, 128:] = total[hi][:, lo : lo + 128].astype(bf16)
    fr[xh, xl] = fs[xh, xl]
    for k, (dh, dx) in enumerate(finals):
        f_wait.append(
            send(
                fs.at[(xh + dh) % nh, (xl + dx) % nx], fr.at[xh, xl],
                f_send.at[k], f_recv.at[k], at_x(dx, 0, dh),
            )
        )

    p_both(len(p_orders[0]))
    x_wait = {}
    for grp in p_orders_last(p_orders):
        lanes = slice(grp * glanes, (grp + 1) * glanes)
        total = parts[y, :, lanes].astype(f32)
        for way in (0, 1):
            if (hy, grp) in p_copies[way]:
                p_copies[way][(hy, grp)].wait_recv()
                total = total + rb[way, hy - 1, :, lanes].astype(f32)
        for xi in range(nx):
            piece = total[xi * rows : (xi + 1) * rows]
            own[xi, :, lanes] = piece
            xs[xi, :, lanes] = piece.astype(bf16)
        for dx in range(1, nx):
            x_wait[(grp, dx)] = send(
                xs.at[(xl + dx) % nx, :, lanes], xr.at[dx - 1, :, lanes],
                x_send.at[grp, dx - 1], x_recv.at[grp, dx - 1], at_x(dx),
            )

    for copy in f_wait:
        copy.wait_recv()
    odd = xl % 2 == 1
    for xi in range(nx):
        total = fr[0, xi].astype(f32)
        for hi in range(1, nh):
            total = total + fr[hi, xi].astype(f32)
        total = total * scale
        last = total[:, 128:]
        last = jnp.where(odd, pltpu.roll(last, 64, 1), last)
        gw_ref[xi * frows : (xi + 1) * frows, :128] = total[:, :128]
        gw_ref[xi * frows : (xi + 1) * frows, 128:] = last[:, :64]

    for grp in p_orders_last(p_orders):
        lanes = slice(grp * glanes, (grp + 1) * glanes)
        total = own[xl, :, lanes]
        for dx in range(1, nx):
            x_wait[(grp, dx)].wait_recv()
            total = total + xr[dx - 1, :, lanes].astype(f32)
        gi_ref[:, lanes] = total.astype(bf16)

    for copy in sent:
        copy.wait_send()


def p_orders_last(orders):
    last = orders[0][-1][0]
    return [g for s, g in orders[0] if s == last] if last > 1 else list(range(GROUPS))


def body(dims, act_codes, scale_exps, weight, grad_out):
    nz, nh, nc, nx, ny = dims["z"], dims["xh"], dims["core"], dims["xl"], dims["y"]
    hy, hz = ny // 2, nz // 2
    rows, width = act_codes.shape
    toks, cols = grad_out.shape
    out_rows = width // (nz * nh * nc)
    feats = width // (nc * nx)
    per = rows * nx
    dcols = nx * cols
    scale = float(1.0 / (toks * nz * nh * nc) ** 0.5)
    bf16, f32 = jnp.bfloat16, jnp.float32
    n_p = GROUPS // 2 + (hy - 1) * GROUPS
    n_z = 1 + (hz - 1) * 2

    def vm(shape, kind=bf16):
        return pltpu.VMEM(shape, kind)

    def sems(*shape):
        return pltpu.SemaphoreType.DMA(shape)

    scratch = [
        vm(act_codes.shape), vm(scale_exps.shape, jnp.int32), vm(weight.shape), vm(grad_out.shape),
        sems(4),
        vm((nx * nc, rows, feats)), vm((nx * nc, rows, feats)), vm((ny, nc, per, feats)),
        vm((feats, nc * toks)), vm((toks, cols)), vm((nc, nx, toks * 3 // 2, 128)),
        vm((nc * toks, 64 * nx)), vm((ny, per, width)), vm((2, hy, per, width)),
        vm((nx, rows, width)), vm((nx - 1, rows, width)), vm((nx, rows, width), f32),
        vm((nz, feats // nz, dcols), f32), vm((nz, feats // nz, dcols)),
        vm((2, hz, feats // nz, dcols)),
        vm((nh, nx, out_rows // nx, 256)), vm((nh, nx, out_rows // nx, 256)),
        sems(nx * nc - 1), sems(nx * nc - 1),
        sems(2, hy * nc), sems(2, hy * nc),
        sems(2 * nx - 1), sems(2 * nx - 1),
        sems(2, n_p), sems(2, n_p),
        sems(2, n_z), sems(2, n_z),
        sems(GROUPS, nx - 1), sems(GROUPS, nx - 1),
        sems(nh * nx - 1), sems(nh * nx - 1),
    ]
    return pl.pallas_call(
        functools.partial(kernel, dims, scale),
        out_shape=(
            jax.ShapeDtypeStruct((rows, width), bf16),
            jax.ShapeDtypeStruct((out_rows, cols), f32),
        ),
        in_specs=[pl.BlockSpec(memory_space=pl.ANY)] * 4,
        out_specs=[pl.BlockSpec(memory_space=pltpu.VMEM)] * 2,
        scratch_shapes=scratch,
        compiler_params=pltpu.CompilerParams(
            collective_id=0, has_side_effects=True, vmem_limit_bytes=48 * 1024 * 1024
        ),
        name="backward",
    )(act_codes, scale_exps, weight, grad_out)


def solution(mesh):
    placed = (P(("ctx", "tp"), None), P(("ctx", "tp"), None), P(None, "tp"), P("ctx", "tp"))
    return jax.shard_map(
        functools.partial(body, DIMS),
        mesh=mesh,
        in_specs=placed,
        out_specs=(P(("ctx", "tp"), None), P("ctx", "tp")),
        check_vma=False,
    )
```

```python
import functools

import jax
import jax.numpy as jnp
from jax import lax
from jax.experimental import pallas as pl
from jax.experimental.pallas import tpu as pltpu
from jax.sharding import PartitionSpec as P

DIMS = {"z": 8, "xh": 2, "core": 2, "xl": 4, "y": 8}
GROUPS = 6
Z_GROUPS = 4
AFTER_AG1, AFTER_AG2, AFTER_Z1, AFTER_Z2 = 3, 3, 4, 5


def ring_pieces(half, groups):
    low, high = tuple(range(groups // 2)), tuple(range(groups // 2, groups))
    ways = []
    for first, rest in ((low, high), (high, low)):
        order = [(1, g) for g in first]
        for step in range(2, half + 1):
            order += [(step, g) for g in rest + first]
        ways.append(order)
    return ways


def kernel(
    dims, scale, codes_hbm, exps_hbm, w_hbm, g_hbm, gi_ref, gw_ref,
    codes, exps, w, wq, wr, g, in_sem,
    s_buf, a1, ab, at, gp, ga, rest, parts, rb, xs, xr, own,
    dwf, dwb, rz, fs, fr, qp, rq, qs, qr,
    s_send, s_recv, a_send, a_recv, g_send, g_recv, p_send, p_recv,
    z_send, z_recv, x_send, x_recv, f_send, f_recv,
    w_send, w_recv, q_send, q_recv, o_send, o_recv,
):
    nz, nh, nc, nx, ny = dims["z"], dims["xh"], dims["core"], dims["xl"], dims["y"]
    hy, hz = ny // 2, nz // 2
    f32, bf16 = jnp.float32, jnp.bfloat16
    ctx, tp = lax.axis_index("ctx"), lax.axis_index("tp")
    z, xh, c = ctx // (nh * nc), (ctx // nc) % nh, ctx % nc
    xl, y = tp // ny, tp % ny

    def at_z(d):
        return {"ctx": ((z + d + nz) % nz * nh + xh) * nc + c, "tp": tp}

    def at_y(d):
        return {"ctx": ctx, "tp": xl * ny + (y + d + ny) % ny}

    def at_x(dx, dc=0, dh=0):
        return {
            "ctx": (z * nh + (xh + dh) % nh) * nc + (c + dc) % nc,
            "tp": (xl + dx) % nx * ny + y,
        }

    rows, width = codes.shape
    cols, toks = g.shape
    blocks = exps.shape[1]
    quarter = 128 // nx
    feats = width // (nc * nx)
    per = rows * nx
    plain = width - 128 * nc * nx
    glanes = plain // GROUPS
    sent = []

    def send(src, dst, ssem, rsem, dev):
        copy = pltpu.make_async_remote_copy(
            src_ref=src, dst_ref=dst, send_sem=ssem, recv_sem=rsem,
            device_id=dev, device_id_type=pl.DeviceIdType.MESH,
        )
        copy.start()
        sent.append(copy)
        return copy

    loads = []
    moves = [(codes_hbm, codes), (exps_hbm, exps), (g_hbm, g), (w_hbm.at[:, :plain], w)]
    for dx in range(nx):
        first = pl.multiple_of(plain + ((xl + dx) % nx * nc + c) * 128, 128)
        moves.append((w_hbm.at[:, pl.ds(first, 128)], wq.at[dx - 1] if dx else wr.at[xl]))
    for i, (src, dst) in enumerate(moves):
        copy = pltpu.make_async_copy(src, dst, in_sem.at[i])
        copy.start()
        loads.append(copy)

    barrier = pltpu.get_barrier_semaphore()
    mates = [(dx, dc) for dx in range(nx) for dc in range(nc) if (dx, dc) != (0, 0)]
    finals = [(dh, dx) for dh in range(nh) for dx in range(nx) if (dh, dx) != (0, 0)]
    peers = [at_x(dx, dc) for dx, dc in mates]
    peers += [at_x(dx, 0, dh) for dh, dx in finals if dh != 0]
    peers += [at_y(d) for d in range(1, ny)]
    peers += [at_z(d) for d in sorted({1, nz - 1, 2 % nz, (nz - 2) % nz} - {0})]
    for dev in peers:
        pl.semaphore_signal(barrier, inc=1, device_id=dev, device_id_type=pl.DeviceIdType.MESH)

    loads[0].wait()
    loads[1].wait()
    scales = jnp.exp2(exps[...].astype(f32))
    lane = lax.broadcasted_iota(jnp.int32, (rows, 128), 1) // quarter
    acts = [
        codes[:, b * 128 : (b + 1) * 128].astype(f32) * scales[:, b : b + 1] for b in range(blocks)
    ]
    for xi in range(nx):
        for ci in range(nc):
            mine = [acts[b] for b in range(blocks) if b % nc == ci]
            for m in range(len(mine) // nx):
                out = mine[m * nx]
                if xi:
                    out = pltpu.roll(out, (128 - xi * quarter) % 128, 1)
                for i in range(1, nx):
                    piece, shift = mine[m * nx + i], ((i - xi) * quarter) % 128
                    if shift:
                        piece = pltpu.roll(piece, shift, 1)
                    out = jnp.where(lane == i, piece, out)
                s_buf[xi * nc + ci, :, m * 128 : (m + 1) * 128] = out.astype(bf16)
    a1[xl * nc + c] = s_buf[xl * nc + c]

    loads[2].wait()
    raw = g[...].astype(f32).T
    raw = jnp.concatenate(
        [
            raw[(i * ny + j) * rows : (i * ny + j + 1) * rows]
            for j in range(ny) for i in range(nx)
        ],
        axis=0,
    )
    gp[...] = raw.astype(bf16)
    ga[c, xl, :toks, :] = raw[:, :128].astype(bf16)
    tail = raw[:, 128:]
    ga[c, xl, toks:, :] = jnp.concatenate([tail[: toks // 2], tail[toks // 2 :]], axis=1).astype(bf16)

    pl.semaphore_wait(barrier, len(peers))

    s_wait = []
    for k, (dx, dc) in enumerate(mates):
        s_wait.append(
            send(
                s_buf.at[(xl + dx) % nx * nc + (c + dc) % nc], a1.at[xl * nc + c],
                s_send.at[k], s_recv.at[k], at_x(dx, dc),
            )
        )
    g_wait = []
    for dx in range(1, nx):
        g_wait.append(
            send(ga.at[c, xl], ga.at[c, xl], g_send.at[dx - 1], g_recv.at[dx - 1], at_x(dx))
        )
    twin_wait = [
        send(ga.at[c, xl], ga.at[c, xl], g_send.at[nx - 1], g_recv.at[nx - 1], at_x(0, 1))
    ]

    w_wait = []
    for dx in range(nx):
        loads[4 + dx].wait()
        if dx:
            w_wait.append(
                send(wq.at[dx - 1], wr.at[xl], w_send.at[dx - 1], w_recv.at[dx - 1], at_x(dx))
            )

    loads[3].wait()
    step_w = min(plain, 512)
    for n in range(plain // step_w):
        part = lax.dot_general(
            gp[...], w[:, n * step_w : (n + 1) * step_w], (((1,), (0,)), ((), ())),
            preferred_element_type=f32,
        )
        parts[:, :, n * step_w : (n + 1) * step_w] = part.astype(bf16).reshape(ny, per, step_w)

    p_orders = ring_pieces(hy, GROUPS)
    p_index = [{piece: i for i, piece in enumerate(order)} for order in p_orders]
    p_copies = [{}, {}]
    p_next = [0, 0]

    def p_piece(way):
        if p_next[way] >= len(p_orders[way]):
            return
        step, grp = p_orders[way][p_next[way]]
        p_next[way] += 1
        sign = 1 - 2 * way
        off = hy + 1 - step
        lanes = slice(grp * glanes, (grp + 1) * glanes)
        dest = (y + sign * off + ny) % ny
        if (step - 1, grp) in p_copies[way]:
            p_copies[way][(step - 1, grp)].wait_recv()
            total = rb[way, step - 2, :, lanes].astype(f32) + parts[dest, :, lanes].astype(f32)
            rb[way, step - 2, :, lanes] = total.astype(bf16)
            src = rb.at[way, step - 2, :, lanes]
        else:
            src = parts.at[dest, :, lanes]
        i = p_index[way][(step, grp)]
        p_copies[way][(step, grp)] = send(
            src, rb.at[way, step - 1, :, lanes], p_send.at[way, i], p_recv.at[way, i], at_y(sign)
        )

    def p_both(count=1):
        for _ in range(count):
            p_piece(0)
            p_piece(1)

    p_both(GROUPS)

    for copy in s_wait:
        copy.wait_recv()
    for ci in range(nc):
        ab[y, ci] = jnp.concatenate(
            [a1[xi * nc + ci].astype(f32) for xi in range(nx)], axis=0
        ).astype(bf16)

    a_copies = [{}, {}]

    def a_piece(way, dist, hops, ci):
        sign = 1 - 2 * way
        ref = ab.at[(y - sign * (dist - hops) + ny) % ny, ci]
        i = (dist - 1) * nc + ci
        a_copies[way][(dist, ci)] = send(
            ref, ref, a_send.at[way, i], a_recv.at[way, i], at_y(sign * hops)
        )

    def a_all(dist, hops):
        for ci in range(nc):
            for way in (0, 1):
                if dist < hy or ci % 2 == way:
                    if dist > 2:
                        a_copies[way][(2, ci)].wait_recv()
                    a_piece(way, dist, hops, ci)

    if hy > 1:
        a_all(2, 2)
    a_all(1, 1)
    p_both(AFTER_AG1)
    if hy > 2:
        a_all(3, 1)
        for ci in range(nc):
            a_piece(ci % 2, 4, 2, ci)
    p_both(AFTER_AG2)

    for dx in range(1, nx):
        g_wait[dx - 1].wait_recv()
        ref = ga.at[c, (xl - dx + nx) % nx]
        twin_wait.append(
            send(ref, ref, g_send.at[nx - 1 + dx], g_recv.at[nx - 1 + dx], at_x(0, 1))
        )

    for way in (0, 1):
        for dist, ci in a_copies[way]:
            if not (dist == 2 and hy > 2):
                a_copies[way][(dist, ci)].wait_recv()
    for ci in range(nc):
        at[:, ci * toks : (ci + 1) * toks] = ab[:, ci].reshape(toks, feats).T
    for copy in twin_wait:
        copy.wait_recv()

    mains = nx * 128
    for ci in range(nc):
        for k in range(nx // 2):
            left = ga[ci, 2 * k, toks:, :].astype(f32)
            right = ga[ci, 2 * k + 1, toks:, :].astype(f32)
            first = lax.broadcasted_iota(jnp.int32, left.shape, 1) < 64
            top = jnp.where(first, left, pltpu.roll(right, 64, 1))
            bottom = jnp.where(first, pltpu.roll(left, 64, 1), right)
            lanes = slice(k * 128, (k + 1) * 128)
            rest[ci * toks : ci * toks + toks // 2, lanes] = top.astype(bf16)
            rest[ci * toks + toks // 2 : (ci + 1) * toks, lanes] = bottom.astype(bf16)
    zrows = feats // nz

    def dw_store(lanes, value):
        value = value.reshape(nz, zrows, value.shape[1])
        dwf[:, :, lanes] = value
        dwb[:, :, lanes] = value.astype(bf16)

    for k in range(nx // 2):
        total = None
        for ci in range(nc):
            both = jnp.concatenate([ga[ci, 2 * k, :toks, :], ga[ci, 2 * k + 1, :toks, :]], axis=1)
            part = jnp.dot(at[:, ci * toks : (ci + 1) * toks], both, preferred_element_type=f32)
            total = part if total is None else total + part
        dw_store(slice(k * 256, (k + 1) * 256), total)
    dw_store(slice(mains, mains + 64 * nx), jnp.dot(at[...], rest[...], preferred_element_type=f32))

    zsub = zrows // Z_GROUPS
    z_copies = [{}, {}]
    halves = [tuple(range(Z_GROUPS // 2)), tuple(range(Z_GROUPS // 2, Z_GROUPS))]

    def z_rows(grp):
        return slice(grp * zsub, (grp + 1) * zsub)

    def z_got(way, slot, grp):
        z_copies[way][(slot, grp)].wait_recv()
        return rz[way, slot, z_rows(grp), :].astype(f32)

    def z_send_piece(way, slot, grp, src, hops):
        i = slot * Z_GROUPS + grp
        z_copies[way][(slot, grp)] = send(
            src, rz.at[way, slot, z_rows(grp), :], z_send.at[way, i], z_recv.at[way, i],
            at_z((1 - 2 * way) * hops),
        )

    def z_round(way, slot, off, grp, arrived):
        dest = (z + (1 - 2 * way) * off + nz) % nz
        if not arrived:
            z_send_piece(way, slot, grp, dwb.at[dest, z_rows(grp), :], 1)
            return
        total = dwf[dest, z_rows(grp), :]
        for old in arrived:
            total = total + z_got(way, old, grp)
        rz[way, arrived[0], z_rows(grp), :] = total.astype(bf16)
        z_send_piece(way, slot, grp, rz.at[way, arrived[0], z_rows(grp), :], 1)

    def z_each(slot, off, has):
        for k in range(Z_GROUPS):
            for way in (0, 1):
                order = halves[1 - way] + halves[way]
                grp = order[k]
                z_round(way, slot, off, grp, has(way, grp))

    if hz == 4:
        for k in range(Z_GROUPS // 2):
            for way in (0, 1):
                grp = halves[way][k]
                dest = (z + (1 - 2 * way) * 4 + nz) % nz
                z_send_piece(way, 0, grp, dwb.at[dest, z_rows(grp), :], 2)
        z_each(1, 3, lambda way, grp: ())
    else:
        for grp in range(Z_GROUPS):
            way = 0 if grp in halves[0] else 1
            z_round(way, 0, hz, grp, ())

    for copy in w_wait:
        copy.wait_recv()
    weights = jnp.concatenate(
        [wr[xi, :128, :] for xi in range(nx)] + [wr[xi, 128:, :] for xi in range(nx)], axis=0
    )
    for ci in range(nc):
        both = jnp.concatenate(
            [ga[ci, xi, :toks, :] for xi in range(nx)] + [rest[ci * toks : (ci + 1) * toks, :]], axis=1
        )
        part = jnp.dot(both, weights, preferred_element_type=f32)
        qp[:, ci] = part.astype(bf16).reshape(ny, per, 128)
    q_wait = []
    for near in range(ny // 2, 0, -1):
        for d in sorted({near, ny - near}):
            q_wait.append(
                send(
                    qp.at[(y + d) % ny], rq.at[d - 1], q_send.at[d - 1], q_recv.at[d - 1], at_y(d)
                )
            )
    p_both(AFTER_Z1)

    if hz == 4:
        z_each(2, 2, lambda way, grp: (1, 0) if grp in halves[way] else (1,))
        p_both(AFTER_Z2)
        z_each(3, 1, lambda way, grp: (2,))
    else:
        for step in range(2, hz + 1):
            z_each(
                step - 1, hz + 1 - step,
                lambda way, grp: (step - 2,) if step > 2 or grp in halves[way] else (),
            )
    p_both(len(p_orders[0]))

    for copy in q_wait:
        copy.wait_recv()
    for ci in range(nc):
        total = qp[y, ci].astype(f32)
        for d in range(1, ny):
            total = total + rq[d - 1, ci].astype(f32)
        for xi in range(nx):
            qs[xi * nc + ci] = total[xi * rows : (xi + 1) * rows].astype(bf16)
    qr[xl * nc + c] = qs[xl * nc + c]
    o_wait = []
    for k, (dx, dc) in enumerate(mates):
        o_wait.append(
            send(
                qs.at[(xl + dx) % nx * nc + (c + dc) % nc], qr.at[xl * nc + c],
                o_send.at[k], o_recv.at[k], at_x(dx, dc),
            )
        )

    f_wait = []
    sums = []
    for grp in range(Z_GROUPS):
        total = dwf[z, z_rows(grp), :]
        for way in (0, 1):
            if (hz - 1, grp) in z_copies[way]:
                total = total + z_got(way, hz - 1, grp)
        sums.append(total)
    some = Z_GROUPS // nh
    total = [jnp.concatenate(sums[hi * some : (hi + 1) * some], axis=0) for hi in range(nh)]
    for hi in range(nh):
        for xi in range(nx):
            fs[hi, xi, :, :128] = total[hi][:, xi * 128 : (xi + 1) * 128].astype(bf16)
            lo = mains + xi // 2 * 128
            fs[hi, xi, :, 128:] = total[hi][:, lo : lo + 128].astype(bf16)
    fr[xh, xl] = fs[xh, xl]
    for k, (dh, dx) in enumerate(finals):
        f_wait.append(
            send(
                fs.at[(xh + dh) % nh, (xl + dx) % nx], fr.at[xh, xl],
                f_send.at[k], f_recv.at[k], at_x(dx, 0, dh),
            )
        )

    x_wait = {}
    for grp in p_orders_last(p_orders):
        lanes = slice(grp * glanes, (grp + 1) * glanes)
        total = parts[y, :, lanes].astype(f32)
        for way in (0, 1):
            if (hy, grp) in p_copies[way]:
                p_copies[way][(hy, grp)].wait_recv()
                total = total + rb[way, hy - 1, :, lanes].astype(f32)
        for xi in range(nx):
            piece = total[xi * rows : (xi + 1) * rows]
            own[xi, :, lanes] = piece
            xs[xi, :, lanes] = piece.astype(bf16)
        for dx in range(1, nx):
            x_wait[(grp, dx)] = send(
                xs.at[(xl + dx) % nx, :, lanes], xr.at[dx - 1, :, lanes],
                x_send.at[grp, dx - 1], x_recv.at[grp, dx - 1], at_x(dx),
            )

    for copy in f_wait:
        copy.wait_recv()
    odd = xl % 2 == 1
    out_rows = []
    for xi in range(nx):
        total = fr[0, xi].astype(f32)
        for hi in range(1, nh):
            total = total + fr[hi, xi].astype(f32)
        out_rows.append(total * scale)
    total = jnp.concatenate(out_rows, axis=0)
    last = total[:, 128:]
    last = jnp.where(odd, pltpu.roll(last, 64, 1), last)
    gw_ref[:128, :] = total[:, :128].T
    gw_ref[128:, :] = last.T[:64]

    for grp in p_orders_last(p_orders):
        lanes = slice(grp * glanes, (grp + 1) * glanes)
        total = own[xl, :, lanes]
        for dx in range(1, nx):
            x_wait[(grp, dx)].wait_recv()
            total = total + xr[dx - 1, :, lanes].astype(f32)
        gi_ref[:, lanes] = total.astype(bf16)

    for copy in o_wait:
        copy.wait_recv()
    for k in range(nx * nc):
        gi_ref[:, plain + k * 128 : plain + (k + 1) * 128] = qr[k]

    for copy in sent:
        copy.wait_send()


def p_orders_last(orders):
    last = orders[0][-1][0]
    return [g for s, g in orders[0] if s == last] if last > 1 else list(range(GROUPS))


def body(dims, act_codes, scale_exps, weight, grad_out):
    weight, grad_out = weight.T, grad_out.T
    act_codes, scale_exps, weight, grad_out = (
        pltpu.with_memory_space_constraint(a, pltpu.HBM) for a in (act_codes, scale_exps, weight, grad_out)
    )
    nz, nh, nc, nx, ny = dims["z"], dims["xh"], dims["core"], dims["xl"], dims["y"]
    hy, hz = ny // 2, nz // 2
    rows, width = act_codes.shape
    cols, toks = grad_out.shape
    out_rows = width // (nz * nh * nc)
    feats = width // (nc * nx)
    per = rows * nx
    dcols = nx * cols
    scale = float(1.0 / (toks * nz * nh * nc) ** 0.5)
    bf16, f32 = jnp.bfloat16, jnp.float32
    n_p = GROUPS // 2 + (hy - 1) * GROUPS
    n_z = hz * Z_GROUPS
    plain = width - 128 * nc * nx

    def vm(shape, kind=bf16):
        return pltpu.VMEM(shape, kind)

    def sems(*shape):
        return pltpu.SemaphoreType.DMA(shape)

    scratch = [
        vm(act_codes.shape), vm(scale_exps.shape, jnp.int32), vm((cols, plain)),
        vm((nx - 1, cols, 128)), vm((nx, cols, 128)), vm(grad_out.shape), sems(4 + nx),
        vm((nx * nc, rows, feats)), vm((nx * nc, rows, feats)), vm((ny, nc, per, feats)),
        vm((feats, nc * toks)), vm((toks, cols)), vm((nc, nx, toks * 3 // 2, 128)),
        vm((nc * toks, 64 * nx)), vm((ny, per, plain)), vm((2, hy, per, plain)),
        vm((nx, rows, plain)), vm((nx - 1, rows, plain)), vm((nx, rows, plain), f32),
        vm((nz, feats // nz, dcols), f32), vm((nz, feats // nz, dcols)),
        vm((2, hz, feats // nz, dcols)),
        vm((nh, nx, out_rows // nx, 256)), vm((nh, nx, out_rows // nx, 256)),
        vm((ny, nc, per, 128)), vm((ny - 1, nc, per, 128)), vm((nx * nc, rows, 128)), vm((nx * nc, rows, 128)),
        sems(nx * nc - 1), sems(nx * nc - 1),
        sems(2, hy * nc), sems(2, hy * nc),
        sems(2 * nx - 1), sems(2 * nx - 1),
        sems(2, n_p), sems(2, n_p),
        sems(2, n_z), sems(2, n_z),
        sems(GROUPS, nx - 1), sems(GROUPS, nx - 1),
        sems(nh * nx - 1), sems(nh * nx - 1),
        sems(nx - 1), sems(nx - 1), sems(ny - 1), sems(ny - 1), sems(nx * nc - 1), sems(nx * nc - 1),
    ]
    grad_input, grad_weight = pl.pallas_call(
        functools.partial(kernel, dims, scale),
        out_shape=(
            jax.ShapeDtypeStruct((rows, width), bf16),
            jax.ShapeDtypeStruct((cols, out_rows), f32),
        ),
        in_specs=[pl.BlockSpec(memory_space=pltpu.HBM)] * 4,
        out_specs=[pl.BlockSpec(memory_space=pltpu.VMEM)] * 2,
        scratch_shapes=scratch,
        compiler_params=pltpu.CompilerParams(
            collective_id=0, has_side_effects=True, vmem_limit_bytes=40 * 1024 * 1024
        ),
        name="backward",
    )(act_codes, scale_exps, weight, grad_out)
    return grad_input, grad_weight.T


def solution(mesh):
    placed = (P(("ctx", "tp"), None), P(("ctx", "tp"), None), P(None, "tp"), P("ctx", "tp"))
    return jax.shard_map(
        functools.partial(body, DIMS),
        mesh=mesh,
        in_specs=placed,
        out_specs=(P(("ctx", "tp"), None), P("ctx", "tp")),
        check_vma=False,
    )
```

```python
import functools

import jax
import jax.numpy as jnp
from jax import lax
from jax.experimental import pallas as pl
from jax.experimental.pallas import tpu as pltpu
from jax.sharding import PartitionSpec as P

DIMS = {"z": 8, "xh": 2, "core": 2, "xl": 4, "y": 8}
GROUPS = 4
Z_GROUPS = 4
SHARED = 256
FIRST, AFTER_AG1, AFTER_AG2, AFTER_Z1, AFTER_Z2 = 6, 0, 4, 2, 2


def ring_pieces(half, groups):
    low, high = tuple(range(groups // 2)), tuple(range(groups // 2, groups))
    ways = []
    for first, rest in ((low, high), (high, low)):
        order = [(1, g) for g in first]
        for step in range(2, half + 1):
            order += [(step, g) for g in rest + first]
        ways.append(order)
    return ways


def kernel(
    dims, scale, codes_hbm, exps_hbm, w_hbm, g_hbm, gi_ref, gw_ref,
    codes, exps, w, wq, wr, g, in_sem,
    s_buf, a1, ab, at, gp, ga, rest, parts, rb, xs, xr, own,
    dwf, dwb, rz, fs, fr, qp, rq, qs, qr,
    s_send, s_recv, a_send, a_recv, g_send, g_recv, p_send, p_recv,
    z_send, z_recv, x_send, x_recv, f_send, f_recv,
    w_send, w_recv, q_send, q_recv, o_send, o_recv,
):
    nz, nh, nc, nx, ny = dims["z"], dims["xh"], dims["core"], dims["xl"], dims["y"]
    hy, hz = ny // 2, nz // 2
    f32, bf16 = jnp.float32, jnp.bfloat16
    ctx, tp = lax.axis_index("ctx"), lax.axis_index("tp")
    z, xh, c = ctx // (nh * nc), (ctx // nc) % nh, ctx % nc
    xl, y = tp // ny, tp % ny

    def at_z(d):
        return {"ctx": ((z + d + nz) % nz * nh + xh) * nc + c, "tp": tp}

    def at_y(d):
        return {"ctx": ctx, "tp": xl * ny + (y + d + ny) % ny}

    def at_x(dx, dc=0, dh=0):
        return {
            "ctx": (z * nh + (xh + dh) % nh) * nc + (c + dc) % nc,
            "tp": (xl + dx) % nx * ny + y,
        }

    rows, width = codes.shape
    cols, toks = g.shape
    blocks = exps.shape[1]
    quarter = 128 // nx
    feats = width // (nc * nx)
    per = rows * nx
    plain = width - SHARED * nc * nx
    glanes = plain // GROUPS
    sent = []

    def send(src, dst, ssem, rsem, dev):
        copy = pltpu.make_async_remote_copy(
            src_ref=src, dst_ref=dst, send_sem=ssem, recv_sem=rsem,
            device_id=dev, device_id_type=pl.DeviceIdType.MESH,
        )
        copy.start()
        sent.append(copy)
        return copy

    loads = []
    moves = [(codes_hbm, codes), (exps_hbm, exps), (g_hbm, g), (w_hbm.at[:, :plain], w)]
    for dx in range(nx):
        first = pl.multiple_of(plain + ((xl + dx) % nx * nc + c) * SHARED, SHARED)
        moves.append((w_hbm.at[:, pl.ds(first, SHARED)], wq.at[dx - 1] if dx else wr.at[xl]))
    for i, (src, dst) in enumerate(moves):
        copy = pltpu.make_async_copy(src, dst, in_sem.at[i])
        copy.start()
        loads.append(copy)

    barrier = pltpu.get_barrier_semaphore()
    mates = [(dx, dc) for dx in range(nx) for dc in range(nc) if (dx, dc) != (0, 0)]
    finals = [(dh, dx) for dh in range(nh)[::-1] for dx in range(nx) if (dh, dx) != (0, 0)]
    peers = [at_x(dx, dc) for dx, dc in mates]
    peers += [at_x(dx, 0, dh) for dh, dx in finals if dh != 0]
    peers += [at_y(d) for d in range(1, ny)]
    peers += [at_z(d) for d in sorted({1, nz - 1, 2 % nz, (nz - 2) % nz} - {0})]
    for dev in peers:
        pl.semaphore_signal(barrier, inc=1, device_id=dev, device_id_type=pl.DeviceIdType.MESH)

    loads[0].wait()
    loads[1].wait()
    scales = jnp.exp2(exps[...].astype(f32))
    lane = lax.broadcasted_iota(jnp.int32, (rows, 128), 1) // quarter
    acts = [
        codes[:, b * 128 : (b + 1) * 128].astype(f32) * scales[:, b : b + 1] for b in range(blocks)
    ]
    for xi in range(nx):
        for ci in range(nc):
            mine = [acts[b] for b in range(blocks) if b % nc == ci]
            for m in range(len(mine) // nx):
                out = mine[m * nx]
                if xi:
                    out = pltpu.roll(out, (128 - xi * quarter) % 128, 1)
                for i in range(1, nx):
                    piece, shift = mine[m * nx + i], ((i - xi) * quarter) % 128
                    if shift:
                        piece = pltpu.roll(piece, shift, 1)
                    out = jnp.where(lane == i, piece, out)
                s_buf[xi * nc + ci, :, m * 128 : (m + 1) * 128] = out.astype(bf16)
    a1[xl * nc + c] = s_buf[xl * nc + c]

    loads[2].wait()
    raw = g[...].astype(f32).T
    raw = jnp.concatenate(
        [
            raw[(i * ny + j) * rows : (i * ny + j + 1) * rows]
            for j in range(ny) for i in range(nx)
        ],
        axis=0,
    )
    gp[...] = raw.astype(bf16)
    ga[c, xl, :toks, :] = raw[:, :128].astype(bf16)
    tail = raw[:, 128:]
    ga[c, xl, toks:, :] = jnp.concatenate([tail[: toks // 2], tail[toks // 2 :]], axis=1).astype(bf16)

    pl.semaphore_wait(barrier, len(peers))

    s_wait = []
    for k, (dx, dc) in enumerate(mates):
        s_wait.append(
            send(
                s_buf.at[(xl + dx) % nx * nc + (c + dc) % nc], a1.at[xl * nc + c],
                s_send.at[k], s_recv.at[k], at_x(dx, dc),
            )
        )
    g_wait = []
    for dx in range(1, nx):
        g_wait.append(
            send(ga.at[c, xl], ga.at[c, xl], g_send.at[dx - 1], g_recv.at[dx - 1], at_x(dx))
        )
    twin_wait = [
        send(ga.at[c, xl], ga.at[c, xl], g_send.at[nx - 1], g_recv.at[nx - 1], at_x(0, 1))
    ]

    w_wait = []
    for dx in range(nx):
        loads[4 + dx].wait()
        if dx:
            w_wait.append(
                send(wq.at[dx - 1], wr.at[xl], w_send.at[dx - 1], w_recv.at[dx - 1], at_x(dx))
            )

    loads[3].wait()
    step_w = min(plain, 512)
    for n in range(plain // step_w):
        part = lax.dot_general(
            gp[...], w[:, n * step_w : (n + 1) * step_w], (((1,), (0,)), ((), ())),
            preferred_element_type=f32,
        )
        parts[:, :, n * step_w : (n + 1) * step_w] = part.astype(bf16).reshape(ny, per, step_w)

    p_orders = ring_pieces(hy, GROUPS)
    p_index = [{piece: i for i, piece in enumerate(order)} for order in p_orders]
    p_copies = [{}, {}]
    p_next = [0, 0]

    def p_piece(way):
        if p_next[way] >= len(p_orders[way]):
            return
        step, grp = p_orders[way][p_next[way]]
        p_next[way] += 1
        sign = 1 - 2 * way
        off = hy + 1 - step
        lanes = slice(grp * glanes, (grp + 1) * glanes)
        dest = (y + sign * off + ny) % ny
        if (step - 1, grp) in p_copies[way]:
            p_copies[way][(step - 1, grp)].wait_recv()
            total = rb[way, step - 2, :, lanes].astype(f32) + parts[dest, :, lanes].astype(f32)
            rb[way, step - 2, :, lanes] = total.astype(bf16)
            src = rb.at[way, step - 2, :, lanes]
        else:
            src = parts.at[dest, :, lanes]
        i = p_index[way][(step, grp)]
        p_copies[way][(step, grp)] = send(
            src, rb.at[way, step - 1, :, lanes], p_send.at[way, i], p_recv.at[way, i], at_y(sign)
        )

    def p_both(count=1):
        for _ in range(count):
            p_piece(0)
            p_piece(1)

    p_both(FIRST)

    for copy in s_wait:
        copy.wait_recv()
    for ci in range(nc):
        ab[y, ci] = jnp.concatenate(
            [a1[xi * nc + ci].astype(f32) for xi in range(nx)], axis=0
        ).astype(bf16)

    a_copies = [{}, {}]

    def a_piece(way, dist, hops, ci):
        sign = 1 - 2 * way
        ref = ab.at[(y - sign * (dist - hops) + ny) % ny, ci]
        i = (dist - 1) * nc + ci
        a_copies[way][(dist, ci)] = send(
            ref, ref, a_send.at[way, i], a_recv.at[way, i], at_y(sign * hops)
        )

    def a_all(dist, hops):
        for ci in range(nc):
            for way in (0, 1):
                if dist < hy or ci % 2 == way:
                    if dist > 2:
                        a_copies[way][(2, ci)].wait_recv()
                    a_piece(way, dist, hops, ci)

    if hy > 1:
        a_all(2, 2)
    a_all(1, 1)
    p_both(AFTER_AG1)
    if hy > 2:
        a_all(3, 1)
        for ci in range(nc):
            a_piece(ci % 2, 4, 2, ci)
    p_both(AFTER_AG2)

    for dx in range(1, nx):
        g_wait[dx - 1].wait_recv()
        ref = ga.at[c, (xl - dx + nx) % nx]
        twin_wait.append(
            send(ref, ref, g_send.at[nx - 1 + dx], g_recv.at[nx - 1 + dx], at_x(0, 1))
        )

    for way in (0, 1):
        for dist, ci in a_copies[way]:
            if not (dist == 2 and hy > 2):
                a_copies[way][(dist, ci)].wait_recv()
    for ci in range(nc):
        at[:, ci * toks : (ci + 1) * toks] = ab[:, ci].reshape(toks, feats).T
    for copy in twin_wait:
        copy.wait_recv()

    mains = nx * 128
    for ci in range(nc):
        for k in range(nx // 2):
            left = ga[ci, 2 * k, toks:, :].astype(f32)
            right = ga[ci, 2 * k + 1, toks:, :].astype(f32)
            first = lax.broadcasted_iota(jnp.int32, left.shape, 1) < 64
            top = jnp.where(first, left, pltpu.roll(right, 64, 1))
            bottom = jnp.where(first, pltpu.roll(left, 64, 1), right)
            lanes = slice(k * 128, (k + 1) * 128)
            rest[ci * toks : ci * toks + toks // 2, lanes] = top.astype(bf16)
            rest[ci * toks + toks // 2 : (ci + 1) * toks, lanes] = bottom.astype(bf16)
    zrows = feats // nz

    def dw_store(lanes, value):
        value = value.reshape(nz, zrows, value.shape[1])
        dwf[:, :, lanes] = value
        dwb[:, :, lanes] = value.astype(bf16)

    for k in range(nx // 2):
        total = None
        for ci in range(nc):
            both = jnp.concatenate([ga[ci, 2 * k, :toks, :], ga[ci, 2 * k + 1, :toks, :]], axis=1)
            part = jnp.dot(at[:, ci * toks : (ci + 1) * toks], both, preferred_element_type=f32)
            total = part if total is None else total + part
        dw_store(slice(k * 256, (k + 1) * 256), total)
    dw_store(slice(mains, mains + 64 * nx), jnp.dot(at[...], rest[...], preferred_element_type=f32))

    zsub = zrows // Z_GROUPS
    z_copies = [{}, {}]
    halves = [tuple(range(Z_GROUPS // 2)), tuple(range(Z_GROUPS // 2, Z_GROUPS))]

    def z_rows(grp):
        return slice(grp * zsub, (grp + 1) * zsub)

    def z_got(way, slot, grp):
        z_copies[way][(slot, grp)].wait_recv()
        return rz[way, slot, z_rows(grp), :].astype(f32)

    def z_send_piece(way, slot, grp, src, hops):
        i = slot * Z_GROUPS + grp
        z_copies[way][(slot, grp)] = send(
            src, rz.at[way, slot, z_rows(grp), :], z_send.at[way, i], z_recv.at[way, i],
            at_z((1 - 2 * way) * hops),
        )

    def z_round(way, slot, off, grp, arrived):
        dest = (z + (1 - 2 * way) * off + nz) % nz
        if not arrived:
            z_send_piece(way, slot, grp, dwb.at[dest, z_rows(grp), :], 1)
            return
        total = dwf[dest, z_rows(grp), :]
        for old in arrived:
            total = total + z_got(way, old, grp)
        rz[way, arrived[0], z_rows(grp), :] = total.astype(bf16)
        z_send_piece(way, slot, grp, rz.at[way, arrived[0], z_rows(grp), :], 1)

    def z_each(slot, off, has):
        for k in range(Z_GROUPS):
            for way in (0, 1):
                order = halves[1 - way] + halves[way]
                grp = order[k]
                z_round(way, slot, off, grp, has(way, grp))

    if hz == 4:
        for k in range(Z_GROUPS // 2):
            for way in (0, 1):
                grp = halves[way][k]
                dest = (z + (1 - 2 * way) * 4 + nz) % nz
                z_send_piece(way, 0, grp, dwb.at[dest, z_rows(grp), :], 2)
        z_each(1, 3, lambda way, grp: ())
    else:
        for grp in range(Z_GROUPS):
            way = 0 if grp in halves[0] else 1
            z_round(way, 0, hz, grp, ())

    for copy in w_wait:
        copy.wait_recv()
    weights = jnp.concatenate(
        [wr[xi, :128, :] for xi in range(nx)] + [wr[xi, 128:, :] for xi in range(nx)], axis=0
    )
    for ci in range(nc):
        both = jnp.concatenate(
            [ga[ci, xi, :toks, :] for xi in range(nx)] + [rest[ci * toks : (ci + 1) * toks, :]], axis=1
        )
        part = jnp.dot(both, weights, preferred_element_type=f32)
        qp[:, ci] = part.astype(bf16).reshape(ny, per, SHARED)
    q_wait = []
    for near in range(ny // 2, 0, -1):
        for d in sorted({near, ny - near}):
            q_wait.append(
                send(
                    qp.at[(y + d) % ny], rq.at[d - 1], q_send.at[d - 1], q_recv.at[d - 1], at_y(d)
                )
            )
    p_both(AFTER_Z1)

    if hz == 4:
        z_each(2, 2, lambda way, grp: (1, 0) if grp in halves[way] else (1,))
        p_both(AFTER_Z2)
        z_each(3, 1, lambda way, grp: (2,))
    else:
        for step in range(2, hz + 1):
            z_each(
                step - 1, hz + 1 - step,
                lambda way, grp: (step - 2,) if step > 2 or grp in halves[way] else (),
            )
    p_both(len(p_orders[0]))

    for copy in q_wait:
        copy.wait_recv()
    for ci in range(nc):
        total = qp[y, ci].astype(f32)
        for d in range(1, ny):
            total = total + rq[d - 1, ci].astype(f32)
        for xi in range(nx):
            qs[xi * nc + ci] = total[xi * rows : (xi + 1) * rows].astype(bf16)
    qr[xl * nc + c] = qs[xl * nc + c]
    o_wait = []
    for k, (dx, dc) in enumerate(mates):
        o_wait.append(
            send(
                qs.at[(xl + dx) % nx * nc + (c + dc) % nc], qr.at[xl * nc + c],
                o_send.at[k], o_recv.at[k], at_x(dx, dc),
            )
        )

    f_wait = []
    sums = []
    for grp in range(Z_GROUPS):
        total = dwf[z, z_rows(grp), :]
        for way in (0, 1):
            if (hz - 1, grp) in z_copies[way]:
                total = total + z_got(way, hz - 1, grp)
        sums.append(total)
    some = Z_GROUPS // nh
    total = [jnp.concatenate(sums[hi * some : (hi + 1) * some], axis=0) for hi in range(nh)]
    for hi in range(nh):
        for xi in range(nx):
            part = total[hi]
            half = part.shape[0] // 2
            fs[hi, xi, : 2 * half, :] = part[:, xi * 128 : (xi + 1) * 128].astype(bf16)
            lo = mains + xi * 64
            last = part[:, lo : lo + 64]
            fs[hi, xi, 2 * half :, :] = jnp.concatenate([last[:half], last[half:]], axis=1).astype(bf16)
    fr[xh, xl] = fs[xh, xl]
    for k, (dh, dx) in enumerate(finals):
        f_wait.append(
            send(
                fs.at[(xh + dh) % nh, (xl + dx) % nx], fr.at[xh, xl],
                f_send.at[k], f_recv.at[k], at_x(dx, 0, dh),
            )
        )

    x_wait = {}
    for grp in p_orders_last(p_orders):
        lanes = slice(grp * glanes, (grp + 1) * glanes)
        total = parts[y, :, lanes].astype(f32)
        for way in (0, 1):
            if (hy, grp) in p_copies[way]:
                p_copies[way][(hy, grp)].wait_recv()
                total = total + rb[way, hy - 1, :, lanes].astype(f32)
        for xi in range(nx):
            piece = total[xi * rows : (xi + 1) * rows]
            own[xi, :, lanes] = piece
            xs[xi, :, lanes] = piece.astype(bf16)
        for dx in range(1, nx):
            x_wait[(grp, dx)] = send(
                xs.at[(xl + dx) % nx, :, lanes], xr.at[dx - 1, :, lanes],
                x_send.at[grp, dx - 1], x_recv.at[grp, dx - 1], at_x(dx),
            )

    for copy in f_wait:
        copy.wait_recv()
    firsts, lasts = [], []
    for xi in range(nx):
        total = fr[0, xi].astype(f32)
        for hi in range(1, nh):
            total = total + fr[hi, xi].astype(f32)
        total = total * scale
        height = total.shape[0] * 2 // 3
        firsts.append(total[:height])
        lasts += [total[height:, :64], total[height:, 64:]]
    gw_ref[:128, :] = jnp.concatenate(firsts, axis=0).T
    gw_ref[128:, :] = jnp.concatenate(lasts, axis=0).T

    for grp in p_orders_last(p_orders):
        lanes = slice(grp * glanes, (grp + 1) * glanes)
        total = own[xl, :, lanes]
        for dx in range(1, nx):
            x_wait[(grp, dx)].wait_recv()
            total = total + xr[dx - 1, :, lanes].astype(f32)
        gi_ref[:, lanes] = total.astype(bf16)

    for copy in o_wait:
        copy.wait_recv()
    for k in range(nx * nc):
        gi_ref[:, plain + k * SHARED : plain + (k + 1) * SHARED] = qr[k]

    for copy in sent:
        copy.wait_send()


def p_orders_last(orders):
    last = orders[0][-1][0]
    return [g for s, g in orders[0] if s == last] if last > 1 else list(range(GROUPS))


def body(dims, act_codes, scale_exps, weight, grad_out):
    weight, grad_out = weight.T, grad_out.T
    act_codes, scale_exps, weight, grad_out = (
        pltpu.with_memory_space_constraint(a, pltpu.HBM) for a in (act_codes, scale_exps, weight, grad_out)
    )
    nz, nh, nc, nx, ny = dims["z"], dims["xh"], dims["core"], dims["xl"], dims["y"]
    hy, hz = ny // 2, nz // 2
    rows, width = act_codes.shape
    cols, toks = grad_out.shape
    out_rows = width // (nz * nh * nc)
    feats = width // (nc * nx)
    per = rows * nx
    dcols = nx * cols
    scale = float(1.0 / (toks * nz * nh * nc) ** 0.5)
    bf16, f32 = jnp.bfloat16, jnp.float32
    n_p = GROUPS // 2 + (hy - 1) * GROUPS
    n_z = hz * Z_GROUPS
    plain = width - SHARED * nc * nx

    def vm(shape, kind=bf16):
        return pltpu.VMEM(shape, kind)

    def sems(*shape):
        return pltpu.SemaphoreType.DMA(shape)

    scratch = [
        vm(act_codes.shape), vm(scale_exps.shape, jnp.int32), vm((cols, plain)),
        vm((nx - 1, cols, SHARED)), vm((nx, cols, SHARED)), vm(grad_out.shape), sems(4 + nx),
        vm((nx * nc, rows, feats)), vm((nx * nc, rows, feats)), vm((ny, nc, per, feats)),
        vm((feats, nc * toks)), vm((toks, cols)), vm((nc, nx, toks * 3 // 2, 128)),
        vm((nc * toks, 64 * nx)), vm((ny, per, plain)), vm((2, hy, per, plain)),
        vm((nx, rows, plain)), vm((nx - 1, rows, plain)), vm((nx, rows, plain), f32),
        vm((nz, feats // nz, dcols), f32), vm((nz, feats // nz, dcols)),
        vm((2, hz, feats // nz, dcols)),
        vm((nh, nx, out_rows // nx * 3 // 2, 128)), vm((nh, nx, out_rows // nx * 3 // 2, 128)),
        vm((ny, nc, per, SHARED)), vm((ny - 1, nc, per, SHARED)),
        vm((nx * nc, rows, SHARED)), vm((nx * nc, rows, SHARED)),
        sems(nx * nc - 1), sems(nx * nc - 1),
        sems(2, hy * nc), sems(2, hy * nc),
        sems(2 * nx - 1), sems(2 * nx - 1),
        sems(2, n_p), sems(2, n_p),
        sems(2, n_z), sems(2, n_z),
        sems(GROUPS, nx - 1), sems(GROUPS, nx - 1),
        sems(nh * nx - 1), sems(nh * nx - 1),
        sems(nx - 1), sems(nx - 1), sems(ny - 1), sems(ny - 1), sems(nx * nc - 1), sems(nx * nc - 1),
    ]
    grad_input, grad_weight = pl.pallas_call(
        functools.partial(kernel, dims, scale),
        out_shape=(
            jax.ShapeDtypeStruct((rows, width), bf16),
            jax.ShapeDtypeStruct((cols, out_rows), f32),
        ),
        in_specs=[pl.BlockSpec(memory_space=pltpu.HBM)] * 4,
        out_specs=[pl.BlockSpec(memory_space=pltpu.VMEM)] * 2,
        scratch_shapes=scratch,
        compiler_params=pltpu.CompilerParams(
            collective_id=0, has_side_effects=True, vmem_limit_bytes=40 * 1024 * 1024
        ),
        name="backward",
    )(act_codes, scale_exps, weight, grad_out)
    return grad_input, grad_weight.T


def solution(mesh):
    placed = (P(("ctx", "tp"), None), P(("ctx", "tp"), None), P(None, "tp"), P("ctx", "tp"))
    return jax.shard_map(
        functools.partial(body, DIMS),
        mesh=mesh,
        in_specs=placed,
        out_specs=(P(("ctx", "tp"), None), P("ctx", "tp")),
        check_vma=False,
    )
```

```python
import functools

import jax
import jax.numpy as jnp
from jax import lax
from jax.experimental import pallas as pl
from jax.experimental.pallas import tpu as pltpu
from jax.sharding import PartitionSpec as P

DIMS = {"z": 8, "xh": 2, "core": 2, "xl": 4, "y": 8}
GROUPS = 4
Z_GROUPS = 2
SHARED = 256
FIRST, AFTER_AG1, AFTER_AG2, AFTER_Z1, AFTER_Z2 = 6, 0, 4, 2, 2


def ring_pieces(half, groups):
    low, high = tuple(range(groups // 2)), tuple(range(groups // 2, groups))
    ways = []
    for first, rest in ((low, high), (high, low)):
        order = [(1, g) for g in first]
        for step in range(2, half + 1):
            order += [(step, g) for g in rest + first]
        ways.append(order)
    return ways


def kernel(
    dims, scale, codes_hbm, exps_hbm, w_hbm, g_hbm, gi_ref, gw_ref,
    codes, exps, w, wq, wr, g, in_sem,
    s_buf, a1, ab, at, gp, ga, rest, parts, rb, xs, xr, own,
    dwf, dwb, rz, fs, fr, qp, rq, qs, qr,
    s_send, s_recv, a_send, a_recv, g_send, g_recv, p_send, p_recv,
    z_send, z_recv, x_send, x_recv, f_send, f_recv,
    w_send, w_recv, q_send, q_recv, o_send, o_recv,
):
    nz, nh, nc, nx, ny = dims["z"], dims["xh"], dims["core"], dims["xl"], dims["y"]
    hy, hz = ny // 2, nz // 2
    f32, bf16 = jnp.float32, jnp.bfloat16
    ctx, tp = lax.axis_index("ctx"), lax.axis_index("tp")
    z, xh, c = ctx // (nh * nc), (ctx // nc) % nh, ctx % nc
    xl, y = tp // ny, tp % ny

    def at_z(d):
        return {"ctx": ((z + d + nz) % nz * nh + xh) * nc + c, "tp": tp}

    def at_y(d):
        return {"ctx": ctx, "tp": xl * ny + (y + d + ny) % ny}

    def at_x(dx, dc=0, dh=0):
        return {
            "ctx": (z * nh + (xh + dh) % nh) * nc + (c + dc) % nc,
            "tp": (xl + dx) % nx * ny + y,
        }

    rows, width = codes.shape
    cols, toks = g.shape
    blocks = exps.shape[1]
    quarter = 128 // nx
    feats = width // (nc * nx)
    pfeats = feats // nh
    per = rows * nx
    plain = width - SHARED * nc * nx
    glanes = plain // GROUPS
    sent = []

    def send(src, dst, ssem, rsem, dev):
        copy = pltpu.make_async_remote_copy(
            src_ref=src, dst_ref=dst, send_sem=ssem, recv_sem=rsem,
            device_id=dev, device_id_type=pl.DeviceIdType.MESH,
        )
        copy.start()
        sent.append(copy)
        return copy

    loads = []
    moves = [(codes_hbm, codes), (exps_hbm, exps), (g_hbm, g), (w_hbm.at[:, :plain], w)]
    for dx in range(nx):
        first = pl.multiple_of(plain + ((xl + dx) % nx * nc + c) * SHARED, SHARED)
        moves.append((w_hbm.at[:, pl.ds(first, SHARED)], wq.at[dx - 1] if dx else wr.at[xl]))
    for i, (src, dst) in enumerate(moves):
        copy = pltpu.make_async_copy(src, dst, in_sem.at[i])
        copy.start()
        loads.append(copy)

    barrier = pltpu.get_barrier_semaphore()
    mates = [(dx, dc) for dx in range(nx) for dc in range(nc) if (dx, dc) != (0, 0)]
    finals = [(dh, dx) for dh in range(nh)[::-1] for dx in range(nx) if (dh, dx) != (0, 0)]
    peers = [at_x(dx, dc) for dx, dc in mates]
    peers += [at_x(dx, 0, dh) for dh, dx in finals if dh != 0]
    peers += [at_y(d) for d in range(1, ny)]
    peers += [at_z(d) for d in sorted({1, nz - 1, 2 % nz, (nz - 2) % nz} - {0})]
    for dev in peers:
        pl.semaphore_signal(barrier, inc=1, device_id=dev, device_id_type=pl.DeviceIdType.MESH)

    loads[0].wait()
    loads[1].wait()
    scales = jnp.exp2(exps[...].astype(f32))
    lane = lax.broadcasted_iota(jnp.int32, (rows, 128), 1) // quarter
    acts = [
        codes[:, b * 128 : (b + 1) * 128].astype(f32) * scales[:, b : b + 1] for b in range(blocks)
    ]
    for xi in range(nx):
        for ci in range(nc):
            mine = []
            for part in range(nh):
                for zi in range(nz):
                    block = acts[(zi * nh + (part + 1) % nh) * nc + ci]
                    if nh == 2:
                        block = jnp.where(xh == 0, block, acts[(zi * nh + part) * nc + ci])
                    mine.append(block)
            for m in range(len(mine) // nx):
                out = mine[m * nx]
                if xi:
                    out = pltpu.roll(out, (128 - xi * quarter) % 128, 1)
                for i in range(1, nx):
                    piece, shift = mine[m * nx + i], ((i - xi) * quarter) % 128
                    if shift:
                        piece = pltpu.roll(piece, shift, 1)
                    out = jnp.where(lane == i, piece, out)
                s_buf[xi * nc + ci, :, m * 128 : (m + 1) * 128] = out.astype(bf16)
    a1[xl * nc + c] = s_buf[xl * nc + c]

    loads[2].wait()
    raw = g[...].astype(f32).T
    raw = jnp.concatenate(
        [
            raw[(i * ny + j) * rows : (i * ny + j + 1) * rows]
            for j in range(ny) for i in range(nx)
        ],
        axis=0,
    )
    gp[...] = raw.astype(bf16)
    ga[c, xl, :toks, :] = raw[:, :128].astype(bf16)
    tail = raw[:, 128:]
    ga[c, xl, toks:, :] = jnp.concatenate([tail[: toks // 2], tail[toks // 2 :]], axis=1).astype(bf16)

    pl.semaphore_wait(barrier, len(peers))

    s_wait = []
    for k, (dx, dc) in enumerate(mates):
        s_wait.append(
            send(
                s_buf.at[(xl + dx) % nx * nc + (c + dc) % nc], a1.at[xl * nc + c],
                s_send.at[k], s_recv.at[k], at_x(dx, dc),
            )
        )
    g_wait = []
    for dx in range(1, nx):
        g_wait.append(
            send(ga.at[c, xl], ga.at[c, xl], g_send.at[dx - 1], g_recv.at[dx - 1], at_x(dx))
        )
    twin_wait = [
        send(ga.at[c, xl], ga.at[c, xl], g_send.at[nx - 1], g_recv.at[nx - 1], at_x(0, 1))
    ]

    w_wait = []
    for dx in range(nx):
        loads[4 + dx].wait()
        if dx:
            w_wait.append(
                send(wq.at[dx - 1], wr.at[xl], w_send.at[dx - 1], w_recv.at[dx - 1], at_x(dx))
            )

    loads[3].wait()
    step_w = min(plain, 512)
    for n in range(plain // step_w):
        part = lax.dot_general(
            gp[...], w[:, n * step_w : (n + 1) * step_w], (((1,), (0,)), ((), ())),
            preferred_element_type=f32,
        )
        parts[:, :, n * step_w : (n + 1) * step_w] = part.astype(bf16).reshape(ny, per, step_w)

    p_orders = ring_pieces(hy, GROUPS)
    p_index = [{piece: i for i, piece in enumerate(order)} for order in p_orders]
    p_copies = [{}, {}]
    p_next = [0, 0]

    def p_piece(way):
        if p_next[way] >= len(p_orders[way]):
            return
        step, grp = p_orders[way][p_next[way]]
        p_next[way] += 1
        sign = 1 - 2 * way
        off = hy + 1 - step
        lanes = slice(grp * glanes, (grp + 1) * glanes)
        dest = (y + sign * off + ny) % ny
        if (step - 1, grp) in p_copies[way]:
            p_copies[way][(step - 1, grp)].wait_recv()
            total = rb[way, step - 2, :, lanes].astype(f32) + parts[dest, :, lanes].astype(f32)
            rb[way, step - 2, :, lanes] = total.astype(bf16)
            src = rb.at[way, step - 2, :, lanes]
        else:
            src = parts.at[dest, :, lanes]
        i = p_index[way][(step, grp)]
        p_copies[way][(step, grp)] = send(
            src, rb.at[way, step - 1, :, lanes], p_send.at[way, i], p_recv.at[way, i], at_y(sign)
        )

    def p_both(count=1):
        for _ in range(count):
            p_piece(0)
            p_piece(1)

    p_both(FIRST)

    for copy in s_wait:
        copy.wait_recv()
    for ci in range(nc):
        block = jnp.concatenate([a1[xi * nc + ci].astype(f32) for xi in range(nx)], axis=0).astype(bf16)
        for part in range(nh):
            ab[y, part, ci] = block[:, part * pfeats : (part + 1) * pfeats]

    a_copies = [{}, {}]

    def a_piece(part, way, dist, hops, ci):
        sign = 1 - 2 * way
        ref = ab.at[(y - sign * (dist - hops) + ny) % ny, part, ci]
        i = ((dist - 1) * nc + ci) * nh + part
        a_copies[way][(part, dist, ci)] = send(
            ref, ref, a_send.at[way, i], a_recv.at[way, i], at_y(sign * hops)
        )

    def a_all(part, dist, hops):
        for ci in range(nc):
            for way in (0, 1):
                if dist < hy or ci % 2 == way:
                    if dist > 2:
                        a_copies[way][(part, 2, ci)].wait_recv()
                    a_piece(part, way, dist, hops, ci)

    def a_wait(part):
        for way in (0, 1):
            for one, dist, ci in a_copies[way]:
                if one == part and not (dist == 2 and hy > 2):
                    a_copies[way][(one, dist, ci)].wait_recv()

    for part in range(nh):
        if hy > 1:
            a_all(part, 2, 2)
        a_all(part, 1, 1)
    p_both(AFTER_AG1)
    if hy > 2:
        for part in range(nh):
            a_all(part, 3, 1)
            for ci in range(nc):
                a_piece(part, ci % 2, 4, 2, ci)
    p_both(AFTER_AG2)

    for dx in range(1, nx):
        g_wait[dx - 1].wait_recv()
        ref = ga.at[c, (xl - dx + nx) % nx]
        twin_wait.append(
            send(ref, ref, g_send.at[nx - 1 + dx], g_recv.at[nx - 1 + dx], at_x(0, 1))
        )

    for copy in twin_wait:
        copy.wait_recv()

    mains = nx * 128
    for ci in range(nc):
        for k in range(nx // 2):
            left = ga[ci, 2 * k, toks:, :].astype(f32)
            right = ga[ci, 2 * k + 1, toks:, :].astype(f32)
            first = lax.broadcasted_iota(jnp.int32, left.shape, 1) < 64
            top = jnp.where(first, left, pltpu.roll(right, 64, 1))
            bottom = jnp.where(first, pltpu.roll(left, 64, 1), right)
            lanes = slice(k * 128, (k + 1) * 128)
            rest[ci * toks : ci * toks + toks // 2, lanes] = top.astype(bf16)
            rest[ci * toks + toks // 2 : (ci + 1) * toks, lanes] = bottom.astype(bf16)
    zrows = pfeats // nz

    def dw_part(part):
        feat = slice(part * pfeats, (part + 1) * pfeats)
        for ci in range(nc):
            at[feat, ci * toks : (ci + 1) * toks] = ab[:, part, ci].reshape(toks, pfeats).T

        def store(lanes, value):
            value = value.reshape(nz, zrows, value.shape[1])
            dwf[part, :, :, lanes] = value
            dwb[part, :, :, lanes] = value.astype(bf16)

        for k in range(nx // 2):
            total = None
            for ci in range(nc):
                both = jnp.concatenate([ga[ci, 2 * k, :toks, :], ga[ci, 2 * k + 1, :toks, :]], axis=1)
                some = jnp.dot(at[feat, ci * toks : (ci + 1) * toks], both, preferred_element_type=f32)
                total = some if total is None else total + some
            store(slice(k * 256, (k + 1) * 256), total)
        store(slice(mains, mains + 64 * nx), jnp.dot(at[feat, :], rest[...], preferred_element_type=f32))

    zsub = zrows // Z_GROUPS
    z_copies = [{}, {}]
    halves = [tuple(range(Z_GROUPS // 2)), tuple(range(Z_GROUPS // 2, Z_GROUPS))]

    def z_rows(grp):
        return slice(grp * zsub, (grp + 1) * zsub)

    def z_got(part, way, slot, grp):
        z_copies[way][(part, slot, grp)].wait_recv()
        return rz[way, slot, part, z_rows(grp), :].astype(f32)

    def z_send_piece(part, way, slot, grp, src, hops):
        i = (slot * nh + part) * Z_GROUPS + grp
        z_copies[way][(part, slot, grp)] = send(
            src, rz.at[way, slot, part, z_rows(grp), :], z_send.at[way, i], z_recv.at[way, i],
            at_z((1 - 2 * way) * hops),
        )

    def z_round(part, way, slot, off, grp, arrived):
        dest = (z + (1 - 2 * way) * off + nz) % nz
        if not arrived:
            z_send_piece(part, way, slot, grp, dwb.at[part, dest, z_rows(grp), :], 1)
            return
        total = dwf[part, dest, z_rows(grp), :]
        for old in arrived:
            total = total + z_got(part, way, old, grp)
        rz[way, arrived[0], part, z_rows(grp), :] = total.astype(bf16)
        z_send_piece(part, way, slot, grp, rz.at[way, arrived[0], part, z_rows(grp), :], 1)

    def z_each(part, slot, off, has):
        for k in range(Z_GROUPS):
            for way in (0, 1):
                order = halves[1 - way] + halves[way]
                grp = order[k]
                z_round(part, way, slot, off, grp, has(way, grp))

    def z_first(part):
        if hz == 4:
            for k in range(Z_GROUPS // 2):
                for way in (0, 1):
                    grp = halves[way][k]
                    dest = (z + (1 - 2 * way) * 4 + nz) % nz
                    z_send_piece(part, way, 0, grp, dwb.at[part, dest, z_rows(grp), :], 2)
            z_each(part, 1, 3, lambda way, grp: ())
        else:
            for grp in range(Z_GROUPS):
                way = 0 if grp in halves[0] else 1
                z_round(part, way, 0, hz, grp, ())

    for part in range(nh):
        a_wait(part)
        dw_part(part)
        z_first(part)

    for copy in w_wait:
        copy.wait_recv()
    weights = jnp.concatenate(
        [wr[xi, :128, :] for xi in range(nx)] + [wr[xi, 128:, :] for xi in range(nx)], axis=0
    )
    for ci in range(nc):
        both = jnp.concatenate(
            [ga[ci, xi, :toks, :] for xi in range(nx)] + [rest[ci * toks : (ci + 1) * toks, :]], axis=1
        )
        part = jnp.dot(both, weights, preferred_element_type=f32)
        qp[:, ci] = part.astype(bf16).reshape(ny, per, SHARED)
    q_wait = []
    for near in range(ny // 2, 0, -1):
        for d in sorted({near, ny - near}):
            q_wait.append(
                send(
                    qp.at[(y + d) % ny], rq.at[d - 1], q_send.at[d - 1], q_recv.at[d - 1], at_y(d)
                )
            )
    p_both(AFTER_Z1)

    if hz == 4:
        for part in range(nh):
            z_each(part, 2, 2, lambda way, grp: (1, 0) if grp in halves[way] else (1,))
        p_both(AFTER_Z2)
        for part in range(nh):
            z_each(part, 3, 1, lambda way, grp: (2,))
    else:
        for step in range(2, hz + 1):
            for part in range(nh):
                z_each(
                    part, step - 1, hz + 1 - step,
                    lambda way, grp: (step - 2,) if step > 2 or grp in halves[way] else (),
                )
    p_both(len(p_orders[0]))

    for copy in q_wait:
        copy.wait_recv()
    for ci in range(nc):
        total = qp[y, ci].astype(f32)
        for d in range(1, ny):
            total = total + rq[d - 1, ci].astype(f32)
        for xi in range(nx):
            qs[xi * nc + ci] = total[xi * rows : (xi + 1) * rows].astype(bf16)
    qr[xl * nc + c] = qs[xl * nc + c]
    o_wait = []
    for k, (dx, dc) in enumerate(mates):
        o_wait.append(
            send(
                qs.at[(xl + dx) % nx * nc + (c + dc) % nc], qr.at[xl * nc + c],
                o_send.at[k], o_recv.at[k], at_x(dx, dc),
            )
        )

    f_wait = []
    for part in range(nh):
        sums = []
        for grp in range(Z_GROUPS):
            total = dwf[part, z, z_rows(grp), :]
            for way in (0, 1):
                if (part, hz - 1, grp) in z_copies[way]:
                    total = total + z_got(part, way, hz - 1, grp)
            sums.append(total)
        total = jnp.concatenate(sums, axis=0)
        half = zrows // 2
        for xi in range(nx):
            fs[part, xi, :zrows, :] = total[:, xi * 128 : (xi + 1) * 128].astype(bf16)
            lo = mains + xi * 64
            last = total[:, lo : lo + 64]
            fs[part, xi, zrows:, :] = jnp.concatenate([last[:half], last[half:]], axis=1).astype(bf16)
        dh = (part + 1) % nh
        if dh == 0:
            fr[xh, xl] = fs[part, xl]
        for k, (far, dx) in enumerate(finals):
            if far == dh:
                f_wait.append(
                    send(
                        fs.at[part, (xl + dx) % nx], fr.at[xh, xl],
                        f_send.at[k], f_recv.at[k], at_x(dx, 0, dh),
                    )
                )

    x_wait = {}
    for grp in p_orders_last(p_orders):
        lanes = slice(grp * glanes, (grp + 1) * glanes)
        total = parts[y, :, lanes].astype(f32)
        for way in (0, 1):
            if (hy, grp) in p_copies[way]:
                p_copies[way][(hy, grp)].wait_recv()
                total = total + rb[way, hy - 1, :, lanes].astype(f32)
        for xi in range(nx):
            piece = total[xi * rows : (xi + 1) * rows]
            own[xi, :, lanes] = piece
            xs[xi, :, lanes] = piece.astype(bf16)
        for dx in range(1, nx):
            x_wait[(grp, dx)] = send(
                xs.at[(xl + dx) % nx, :, lanes], xr.at[dx - 1, :, lanes],
                x_send.at[grp, dx - 1], x_recv.at[grp, dx - 1], at_x(dx),
            )

    for copy in f_wait:
        copy.wait_recv()
    firsts, lasts = [], []
    for xi in range(nx):
        total = fr[0, xi].astype(f32)
        for hi in range(1, nh):
            total = total + fr[hi, xi].astype(f32)
        total = total * scale
        height = total.shape[0] * 2 // 3
        firsts.append(total[:height])
        lasts += [total[height:, :64], total[height:, 64:]]
    gw_ref[:128, :] = jnp.concatenate(firsts, axis=0).T
    gw_ref[128:, :] = jnp.concatenate(lasts, axis=0).T

    for grp in p_orders_last(p_orders):
        lanes = slice(grp * glanes, (grp + 1) * glanes)
        total = own[xl, :, lanes]
        for dx in range(1, nx):
            x_wait[(grp, dx)].wait_recv()
            total = total + xr[dx - 1, :, lanes].astype(f32)
        gi_ref[:, lanes] = total.astype(bf16)

    for copy in o_wait:
        copy.wait_recv()
    for k in range(nx * nc):
        gi_ref[:, plain + k * SHARED : plain + (k + 1) * SHARED] = qr[k]

    for copy in sent:
        copy.wait_send()


def p_orders_last(orders):
    last = orders[0][-1][0]
    return [g for s, g in orders[0] if s == last] if last > 1 else list(range(GROUPS))


def body(dims, act_codes, scale_exps, weight, grad_out):
    weight, grad_out = weight.T, grad_out.T
    act_codes, scale_exps, weight, grad_out = (
        pltpu.with_memory_space_constraint(a, pltpu.HBM) for a in (act_codes, scale_exps, weight, grad_out)
    )
    nz, nh, nc, nx, ny = dims["z"], dims["xh"], dims["core"], dims["xl"], dims["y"]
    hy, hz = ny // 2, nz // 2
    rows, width = act_codes.shape
    cols, toks = grad_out.shape
    out_rows = width // (nz * nh * nc)
    feats = width // (nc * nx)
    per = rows * nx
    dcols = nx * cols
    scale = float(1.0 / (toks * nz * nh * nc) ** 0.5)
    bf16, f32 = jnp.bfloat16, jnp.float32
    n_p = GROUPS // 2 + (hy - 1) * GROUPS
    n_z = hz * nh * Z_GROUPS
    plain = width - SHARED * nc * nx

    def vm(shape, kind=bf16):
        return pltpu.VMEM(shape, kind)

    def sems(*shape):
        return pltpu.SemaphoreType.DMA(shape)

    scratch = [
        vm(act_codes.shape), vm(scale_exps.shape, jnp.int32), vm((cols, plain)),
        vm((nx - 1, cols, SHARED)), vm((nx, cols, SHARED)), vm(grad_out.shape), sems(4 + nx),
        vm((nx * nc, rows, feats)), vm((nx * nc, rows, feats)), vm((ny, nh, nc, per, feats // nh)),
        vm((feats, nc * toks)), vm((toks, cols)), vm((nc, nx, toks * 3 // 2, 128)),
        vm((nc * toks, 64 * nx)), vm((ny, per, plain)), vm((2, hy, per, plain)),
        vm((nx, rows, plain)), vm((nx - 1, rows, plain)), vm((nx, rows, plain), f32),
        vm((nh, nz, feats // nh // nz, dcols), f32), vm((nh, nz, feats // nh // nz, dcols)),
        vm((2, hz, nh, feats // nh // nz, dcols)),
        vm((nh, nx, out_rows // nx * 3 // 2, 128)), vm((nh, nx, out_rows // nx * 3 // 2, 128)),
        vm((ny, nc, per, SHARED)), vm((ny - 1, nc, per, SHARED)),
        vm((nx * nc, rows, SHARED)), vm((nx * nc, rows, SHARED)),
        sems(nx * nc - 1), sems(nx * nc - 1),
        sems(2, hy * nc * nh), sems(2, hy * nc * nh),
        sems(2 * nx - 1), sems(2 * nx - 1),
        sems(2, n_p), sems(2, n_p),
        sems(2, n_z), sems(2, n_z),
        sems(GROUPS, nx - 1), sems(GROUPS, nx - 1),
        sems(nh * nx - 1), sems(nh * nx - 1),
        sems(nx - 1), sems(nx - 1), sems(ny - 1), sems(ny - 1), sems(nx * nc - 1), sems(nx * nc - 1),
    ]
    grad_input, grad_weight = pl.pallas_call(
        functools.partial(kernel, dims, scale),
        out_shape=(
            jax.ShapeDtypeStruct((rows, width), bf16),
            jax.ShapeDtypeStruct((cols, out_rows), f32),
        ),
        in_specs=[pl.BlockSpec(memory_space=pltpu.HBM)] * 4,
        out_specs=[pl.BlockSpec(memory_space=pltpu.VMEM)] * 2,
        scratch_shapes=scratch,
        compiler_params=pltpu.CompilerParams(
            collective_id=0, has_side_effects=True, vmem_limit_bytes=40 * 1024 * 1024
        ),
        name="backward",
    )(act_codes, scale_exps, weight, grad_out)
    return grad_input, grad_weight.T


def solution(mesh):
    placed = (P(("ctx", "tp"), None), P(("ctx", "tp"), None), P(None, "tp"), P("ctx", "tp"))
    return jax.shard_map(
        functools.partial(body, DIMS),
        mesh=mesh,
        in_specs=placed,
        out_specs=(P(("ctx", "tp"), None), P("ctx", "tp")),
        check_vma=False,
    )
```

```python
import functools
import math

import jax
import jax.numpy as jnp
from jax import lax
from jax.experimental import pallas as pl
from jax.experimental.pallas import tpu as pltpu
from jax.sharding import PartitionSpec as P

DIMS = {"z": 8, "xh": 2, "core": 2, "xl": 4, "y": 8}
GROUPS = 4
Z_GROUPS = 2
SHARED = 256
FIRST, AFTER_AG1, AFTER_AG2, AFTER_Z1, AFTER_Z2 = 6, 0, 4, 2, 2


def ring_pieces(half, groups):
    low, high = tuple(range(groups // 2)), tuple(range(groups // 2, groups))
    ways = []
    for first, rest in ((low, high), (high, low)):
        order = [(1, g) for g in first]
        for step in range(2, half + 1):
            order += [(step, g) for g in rest + first]
        ways.append(order)
    return ways


def kernel(
    dims, scale, codes_hbm, exps_hbm, w_hbm, g_hbm, gi_out, gw_out,
    gi_ref, gw_ref, out_sem,
    codes, exps, w, wq, wr, g, in_sem,
    s_buf, a1, ab, at, gp, ga, rest, parts, rb, xs, xr, own,
    dwf, dwb, rz, fs, fr, qp, rq, qs, qr,
    gone, filler, s_recv, a_recv, g_recv, p_recv, z_recv, x_recv, f_recv, w_recv, q_recv, o_recv,
):
    nz, nh, nc, nx, ny = dims["z"], dims["xh"], dims["core"], dims["xl"], dims["y"]
    hy, hz = ny // 2, nz // 2
    f32, bf16 = jnp.float32, jnp.bfloat16
    ctx, tp = lax.axis_index("ctx"), lax.axis_index("tp")
    z, xh, c = ctx // (nh * nc), (ctx // nc) % nh, ctx % nc
    xl, y = tp // ny, tp % ny

    def at_z(d):
        return {"ctx": ((z + d + nz) % nz * nh + xh) * nc + c, "tp": tp}

    def at_y(d):
        return {"ctx": ctx, "tp": xl * ny + (y + d + ny) % ny}

    def at_x(dx, dc=0, dh=0):
        return {
            "ctx": (z * nh + (xh + dh) % nh) * nc + (c + dc) % nc,
            "tp": (xl + dx) % nx * ny + y,
        }

    rows, width = codes.shape
    cols, toks = g.shape
    blocks = exps.shape[1]
    quarter = 128 // nx
    feats = width // (nc * nx)
    pfeats = feats // nh
    per = rows * nx
    plain = width - SHARED * nc * nx
    glanes = plain // GROUPS
    sent = {}

    def send(src, dst, kind, rsem, dev):
        copy = pltpu.make_async_remote_copy(
            src_ref=src, dst_ref=dst, send_sem=gone.at[kind], recv_sem=rsem,
            device_id=dev, device_id_type=pl.DeviceIdType.MESH,
        )
        copy.start()
        sent[kind] = sent.get(kind, 0) + math.prod(src.shape)
        return copy

    loads = []
    moves = [(codes_hbm, codes), (exps_hbm, exps), (g_hbm, g), (w_hbm.at[:, :plain], w)]
    for dx in range(nx):
        first = pl.multiple_of(plain + ((xl + dx) % nx * nc + c) * SHARED, SHARED)
        moves.append((w_hbm.at[:, pl.ds(first, SHARED)], wq.at[dx - 1] if dx else wr.at[xl]))
    for i, (src, dst) in enumerate(moves):
        copy = pltpu.make_async_copy(src, dst, in_sem.at[i])
        copy.start()
        loads.append(copy)

    barrier = pltpu.get_barrier_semaphore()
    mates = [(dx, dc) for dx in range(nx) for dc in range(nc) if (dx, dc) != (0, 0)]
    finals = [(dh, dx) for dh in range(nh)[::-1] for dx in range(nx) if (dh, dx) != (0, 0)]
    peers = [at_x(dx, dc) for dx, dc in mates]
    peers += [at_x(dx, 0, dh) for dh, dx in finals if dh != 0]
    peers += [at_y(d) for d in range(1, ny)]
    peers += [at_z(d) for d in sorted({1, nz - 1, 2 % nz, (nz - 2) % nz} - {0})]
    for dev in peers:
        pl.semaphore_signal(barrier, inc=1, device_id=dev, device_id_type=pl.DeviceIdType.MESH)

    loads[0].wait()
    loads[1].wait()
    scales = jnp.exp2(exps[...].astype(f32))
    lane = lax.broadcasted_iota(jnp.int32, (rows, 128), 1) // quarter
    acts = [
        codes[:, b * 128 : (b + 1) * 128].astype(f32) * scales[:, b : b + 1] for b in range(blocks)
    ]
    for xi in range(nx):
        for ci in range(nc):
            mine = []
            for part in range(nh):
                for zi in range(nz):
                    block = acts[(zi * nh + (part + 1) % nh) * nc + ci]
                    if nh == 2:
                        block = jnp.where(xh == 0, block, acts[(zi * nh + part) * nc + ci])
                    mine.append(block)
            for m in range(len(mine) // nx):
                out = mine[m * nx]
                if xi:
                    out = pltpu.roll(out, (128 - xi * quarter) % 128, 1)
                for i in range(1, nx):
                    piece, shift = mine[m * nx + i], ((i - xi) * quarter) % 128
                    if shift:
                        piece = pltpu.roll(piece, shift, 1)
                    out = jnp.where(lane == i, piece, out)
                s_buf[xi * nc + ci, :, m * 128 : (m + 1) * 128] = out.astype(bf16)
    a1[xl * nc + c] = s_buf[xl * nc + c]

    loads[2].wait()
    raw = g[...].astype(f32).T
    raw = jnp.concatenate(
        [
            raw[(i * ny + j) * rows : (i * ny + j + 1) * rows]
            for j in range(ny) for i in range(nx)
        ],
        axis=0,
    )
    gp[...] = raw.astype(bf16)
    ga[c, xl, :toks, :] = raw[:, :128].astype(bf16)
    tail = raw[:, 128:]
    ga[c, xl, toks:, :] = jnp.concatenate([tail[: toks // 2], tail[toks // 2 :]], axis=1).astype(bf16)

    pl.semaphore_wait(barrier, len(peers))

    s_wait = []
    for k, (dx, dc) in enumerate(mates):
        s_wait.append(
            send(
                s_buf.at[(xl + dx) % nx * nc + (c + dc) % nc], a1.at[xl * nc + c],
                0, s_recv.at[k], at_x(dx, dc),
            )
        )
    g_wait = []
    for dx in range(1, nx):
        g_wait.append(
            send(ga.at[c, xl], ga.at[c, xl], 2, g_recv.at[dx - 1], at_x(dx))
        )
    twin_wait = [
        send(ga.at[c, xl], ga.at[c, xl], 2, g_recv.at[nx - 1], at_x(0, 1))
    ]

    w_wait = []
    for dx in range(nx):
        loads[4 + dx].wait()
        if dx:
            w_wait.append(
                send(wq.at[dx - 1], wr.at[xl], 7, w_recv.at[dx - 1], at_x(dx))
            )

    loads[3].wait()
    step_w = min(plain, 512)
    for n in range(plain // step_w):
        part = lax.dot_general(
            gp[...], w[:, n * step_w : (n + 1) * step_w], (((1,), (0,)), ((), ())),
            preferred_element_type=f32,
        )
        parts[:, :, n * step_w : (n + 1) * step_w] = part.astype(bf16).reshape(ny, per, step_w)

    p_orders = ring_pieces(hy, GROUPS)
    p_index = [{piece: i for i, piece in enumerate(order)} for order in p_orders]
    p_copies = [{}, {}]
    p_next = [0, 0]

    def p_piece(way):
        if p_next[way] >= len(p_orders[way]):
            return
        step, grp = p_orders[way][p_next[way]]
        p_next[way] += 1
        sign = 1 - 2 * way
        off = hy + 1 - step
        lanes = slice(grp * glanes, (grp + 1) * glanes)
        dest = (y + sign * off + ny) % ny
        if (step - 1, grp) in p_copies[way]:
            p_copies[way][(step - 1, grp)].wait_recv()
            total = rb[way, step - 2, :, lanes].astype(f32) + parts[dest, :, lanes].astype(f32)
            rb[way, step - 2, :, lanes] = total.astype(bf16)
            src = rb.at[way, step - 2, :, lanes]
        else:
            src = parts.at[dest, :, lanes]
        i = p_index[way][(step, grp)]
        p_copies[way][(step, grp)] = send(
            src, rb.at[way, step - 1, :, lanes], 3, p_recv.at[way, i], at_y(sign)
        )

    def p_both(count=1):
        for _ in range(count):
            p_piece(0)
            p_piece(1)

    p_both(FIRST)

    for copy in s_wait:
        copy.wait_recv()
    for ci in range(nc):
        block = jnp.concatenate([a1[xi * nc + ci].astype(f32) for xi in range(nx)], axis=0).astype(bf16)
        for part in range(nh):
            ab[y, part, ci] = block[:, part * pfeats : (part + 1) * pfeats]

    a_copies = [{}, {}]

    def a_piece(part, way, dist, hops, ci):
        sign = 1 - 2 * way
        ref = ab.at[(y - sign * (dist - hops) + ny) % ny, part, ci]
        i = ((dist - 1) * nc + ci) * nh + part
        a_copies[way][(part, dist, ci)] = send(
            ref, ref, 1, a_recv.at[way, i], at_y(sign * hops)
        )

    def a_all(part, dist, hops):
        for ci in range(nc):
            for way in (0, 1):
                if dist < hy or ci % 2 == way:
                    if dist > 2:
                        a_copies[way][(part, 2, ci)].wait_recv()
                    a_piece(part, way, dist, hops, ci)

    def a_wait(part):
        for way in (0, 1):
            for one, dist, ci in a_copies[way]:
                if one == part and not (dist == 2 and hy > 2):
                    a_copies[way][(one, dist, ci)].wait_recv()

    for part in range(nh):
        if hy > 1:
            a_all(part, 2, 2)
        a_all(part, 1, 1)
    p_both(AFTER_AG1)
    if hy > 2:
        for part in range(nh):
            a_all(part, 3, 1)
            for ci in range(nc):
                a_piece(part, ci % 2, 4, 2, ci)
    p_both(AFTER_AG2)

    for dx in range(1, nx):
        g_wait[dx - 1].wait_recv()
        ref = ga.at[c, (xl - dx + nx) % nx]
        twin_wait.append(
            send(ref, ref, 2, g_recv.at[nx - 1 + dx], at_x(0, 1))
        )

    for copy in twin_wait:
        copy.wait_recv()

    mains = nx * 128
    for ci in range(nc):
        for k in range(nx // 2):
            left = ga[ci, 2 * k, toks:, :].astype(f32)
            right = ga[ci, 2 * k + 1, toks:, :].astype(f32)
            first = lax.broadcasted_iota(jnp.int32, left.shape, 1) < 64
            top = jnp.where(first, left, pltpu.roll(right, 64, 1))
            bottom = jnp.where(first, pltpu.roll(left, 64, 1), right)
            lanes = slice(k * 128, (k + 1) * 128)
            rest[ci * toks : ci * toks + toks // 2, lanes] = top.astype(bf16)
            rest[ci * toks + toks // 2 : (ci + 1) * toks, lanes] = bottom.astype(bf16)
    zrows = pfeats // nz

    def dw_part(part):
        feat = slice(part * pfeats, (part + 1) * pfeats)
        for ci in range(nc):
            at[feat, ci * toks : (ci + 1) * toks] = ab[:, part, ci].reshape(toks, pfeats).T

        def store(lanes, value):
            value = value.reshape(nz, zrows, value.shape[1])
            dwf[part, :, :, lanes] = value
            dwb[part, :, :, lanes] = value.astype(bf16)

        for k in range(nx // 2):
            total = None
            for ci in range(nc):
                both = jnp.concatenate([ga[ci, 2 * k, :toks, :], ga[ci, 2 * k + 1, :toks, :]], axis=1)
                some = jnp.dot(at[feat, ci * toks : (ci + 1) * toks], both, preferred_element_type=f32)
                total = some if total is None else total + some
            store(slice(k * 256, (k + 1) * 256), total)
        store(slice(mains, mains + 64 * nx), jnp.dot(at[feat, :], rest[...], preferred_element_type=f32))

    zsub = zrows // Z_GROUPS
    z_copies = [{}, {}]
    halves = [tuple(range(Z_GROUPS // 2)), tuple(range(Z_GROUPS // 2, Z_GROUPS))]

    def z_rows(grp):
        return slice(grp * zsub, (grp + 1) * zsub)

    def z_got(part, way, slot, grp):
        z_copies[way][(part, slot, grp)].wait_recv()
        return rz[way, slot, part, z_rows(grp), :].astype(f32)

    def z_send_piece(part, way, slot, grp, src, hops):
        i = (slot * nh + part) * Z_GROUPS + grp
        z_copies[way][(part, slot, grp)] = send(
            src, rz.at[way, slot, part, z_rows(grp), :], 4, z_recv.at[way, i],
            at_z((1 - 2 * way) * hops),
        )

    def z_round(part, way, slot, off, grp, arrived):
        dest = (z + (1 - 2 * way) * off + nz) % nz
        if not arrived:
            z_send_piece(part, way, slot, grp, dwb.at[part, dest, z_rows(grp), :], 1)
            return
        total = dwf[part, dest, z_rows(grp), :]
        for old in arrived:
            total = total + z_got(part, way, old, grp)
        rz[way, arrived[0], part, z_rows(grp), :] = total.astype(bf16)
        z_send_piece(part, way, slot, grp, rz.at[way, arrived[0], part, z_rows(grp), :], 1)

    def z_each(part, slot, off, has):
        for k in range(Z_GROUPS):
            for way in (0, 1):
                order = halves[1 - way] + halves[way]
                grp = order[k]
                z_round(part, way, slot, off, grp, has(way, grp))

    def z_first(part):
        if hz == 4:
            for k in range(Z_GROUPS // 2):
                for way in (0, 1):
                    grp = halves[way][k]
                    dest = (z + (1 - 2 * way) * 4 + nz) % nz
                    z_send_piece(part, way, 0, grp, dwb.at[part, dest, z_rows(grp), :], 2)
            z_each(part, 1, 3, lambda way, grp: ())
        else:
            for grp in range(Z_GROUPS):
                way = 0 if grp in halves[0] else 1
                z_round(part, way, 0, hz, grp, ())

    for part in range(nh):
        a_wait(part)
        dw_part(part)
        z_first(part)

    for copy in w_wait:
        copy.wait_recv()
    weights = jnp.concatenate(
        [wr[xi, :128, :] for xi in range(nx)] + [wr[xi, 128:, :] for xi in range(nx)], axis=0
    )
    for ci in range(nc):
        both = jnp.concatenate(
            [ga[ci, xi, :toks, :] for xi in range(nx)] + [rest[ci * toks : (ci + 1) * toks, :]], axis=1
        )
        part = jnp.dot(both, weights, preferred_element_type=f32)
        qp[:, ci] = part.astype(bf16).reshape(ny, per, SHARED)
    q_wait = []
    for near in range(ny // 2, 0, -1):
        for d in sorted({near, ny - near}):
            q_wait.append(
                send(
                    qp.at[(y + d) % ny], rq.at[d - 1], 8, q_recv.at[d - 1], at_y(d)
                )
            )
    p_both(AFTER_Z1)

    if hz == 4:
        for part in range(nh):
            z_each(part, 2, 2, lambda way, grp: (1, 0) if grp in halves[way] else (1,))
        p_both(AFTER_Z2)
        for part in range(nh):
            z_each(part, 3, 1, lambda way, grp: (2,))
    else:
        for step in range(2, hz + 1):
            for part in range(nh):
                z_each(
                    part, step - 1, hz + 1 - step,
                    lambda way, grp: (step - 2,) if step > 2 or grp in halves[way] else (),
                )
    p_both(len(p_orders[0]))

    for copy in q_wait:
        copy.wait_recv()
    for ci in range(nc):
        total = qp[y, ci].astype(f32)
        for d in range(1, ny):
            total = total + rq[d - 1, ci].astype(f32)
        for xi in range(nx):
            qs[xi * nc + ci] = total[xi * rows : (xi + 1) * rows].astype(bf16)
    qr[xl * nc + c] = qs[xl * nc + c]
    o_wait = []
    for k, (dx, dc) in enumerate(mates):
        o_wait.append(
            send(
                qs.at[(xl + dx) % nx * nc + (c + dc) % nc], qr.at[xl * nc + c],
                9, o_recv.at[k], at_x(dx, dc),
            )
        )

    f_wait = []
    for part in range(nh):
        sums = []
        for grp in range(Z_GROUPS):
            total = dwf[part, z, z_rows(grp), :]
            for way in (0, 1):
                if (part, hz - 1, grp) in z_copies[way]:
                    total = total + z_got(part, way, hz - 1, grp)
            sums.append(total)
        total = jnp.concatenate(sums, axis=0)
        half = zrows // 2
        for xi in range(nx):
            fs[part, xi, :zrows, :] = total[:, xi * 128 : (xi + 1) * 128].astype(bf16)
            lo = mains + xi * 64
            last = total[:, lo : lo + 64]
            fs[part, xi, zrows:, :] = jnp.concatenate([last[:half], last[half:]], axis=1).astype(bf16)
        dh = (part + 1) % nh
        if dh == 0:
            fr[xh, xl] = fs[part, xl]
        for k, (far, dx) in enumerate(finals):
            if far == dh:
                f_wait.append(
                    send(
                        fs.at[part, (xl + dx) % nx], fr.at[xh, xl],
                        6, f_recv.at[k], at_x(dx, 0, dh),
                    )
                )

    x_wait = {}
    for grp in p_orders_last(p_orders):
        lanes = slice(grp * glanes, (grp + 1) * glanes)
        total = parts[y, :, lanes].astype(f32)
        for way in (0, 1):
            if (hy, grp) in p_copies[way]:
                p_copies[way][(hy, grp)].wait_recv()
                total = total + rb[way, hy - 1, :, lanes].astype(f32)
        for xi in range(nx):
            piece = total[xi * rows : (xi + 1) * rows]
            own[xi, :, lanes] = piece
            xs[xi, :, lanes] = piece.astype(bf16)
        for dx in range(1, nx):
            x_wait[(grp, dx)] = send(
                xs.at[(xl + dx) % nx, :, lanes], xr.at[dx - 1, :, lanes],
                5, x_recv.at[grp, dx - 1], at_x(dx),
            )

    for copy in f_wait:
        copy.wait_recv()
    firsts, lasts = [], []
    for xi in range(nx):
        total = fr[0, xi].astype(f32)
        for hi in range(1, nh):
            total = total + fr[hi, xi].astype(f32)
        total = total * scale
        height = total.shape[0] * 2 // 3
        firsts.append(total[:height])
        lasts += [total[height:, :64], total[height:, 64:]]
    gw_ref[:128, :] = jnp.concatenate(firsts, axis=0).T
    gw_ref[128:, :] = jnp.concatenate(lasts, axis=0).T
    outs = [pltpu.make_async_copy(gw_ref, gw_out, out_sem.at[0])]
    outs[0].start()

    def put(first, size, i):
        lanes = pl.ds(first, size)
        copy = pltpu.make_async_copy(gi_ref.at[:, lanes], gi_out.at[:, lanes], out_sem.at[i])
        copy.start()
        outs.append(copy)

    for copy in o_wait:
        copy.wait_recv()
    for k in range(nx * nc):
        gi_ref[:, plain + k * SHARED : plain + (k + 1) * SHARED] = qr[k]
    put(plain, width - plain, 1)

    for grp in p_orders_last(p_orders):
        lanes = slice(grp * glanes, (grp + 1) * glanes)
        total = own[xl, :, lanes]
        for dx in range(1, nx):
            x_wait[(grp, dx)].wait_recv()
            total = total + xr[dx - 1, :, lanes].astype(f32)
        gi_ref[:, lanes] = total.astype(bf16)
        put(grp * glanes, glanes, 2 + grp)

    for kind, size in sent.items():
        same = filler.at[pl.ds(0, size // 128), :]
        pltpu.make_async_copy(same, same, gone.at[kind]).wait()
    for copy in outs:
        copy.wait()


def p_orders_last(orders):
    last = orders[0][-1][0]
    return [g for s, g in orders[0] if s == last] if last > 1 else list(range(GROUPS))


def body(dims, act_codes, scale_exps, weight, grad_out):
    weight, grad_out = weight.T, grad_out.T
    act_codes, scale_exps, weight, grad_out = (
        pltpu.with_memory_space_constraint(a, pltpu.HBM) for a in (act_codes, scale_exps, weight, grad_out)
    )
    nz, nh, nc, nx, ny = dims["z"], dims["xh"], dims["core"], dims["xl"], dims["y"]
    hy, hz = ny // 2, nz // 2
    rows, width = act_codes.shape
    cols, toks = grad_out.shape
    out_rows = width // (nz * nh * nc)
    feats = width // (nc * nx)
    per = rows * nx
    dcols = nx * cols
    scale = float(1.0 / (toks * nz * nh * nc) ** 0.5)
    bf16, f32 = jnp.bfloat16, jnp.float32
    n_p = GROUPS // 2 + (hy - 1) * GROUPS
    n_z = hz * nh * Z_GROUPS
    plain = width - SHARED * nc * nx

    def vm(shape, kind=bf16):
        return pltpu.VMEM(shape, kind)

    def sems(*shape):
        return pltpu.SemaphoreType.DMA(shape)

    scratch = [
        vm(act_codes.shape), vm((cols, out_rows), f32), sems(2 + GROUPS),
        vm(act_codes.shape), vm(scale_exps.shape, jnp.int32), vm((cols, plain)),
        vm((nx - 1, cols, SHARED)), vm((nx, cols, SHARED)), vm(grad_out.shape), sems(4 + nx),
        vm((nx * nc, rows, feats)), vm((nx * nc, rows, feats)), vm((ny, nh, nc, per, feats // nh)),
        vm((feats, nc * toks)), vm((toks, cols)), vm((nc, nx, toks * 3 // 2, 128)),
        vm((nc * toks, 64 * nx)), vm((ny, per, plain)), vm((2, hy, per, plain)),
        vm((nx, rows, plain)), vm((nx - 1, rows, plain)), vm((nx, rows, plain), f32),
        vm((nh, nz, feats // nh // nz, dcols), f32), vm((nh, nz, feats // nh // nz, dcols)),
        vm((2, hz, nh, feats // nh // nz, dcols)),
        vm((nh, nx, out_rows // nx * 3 // 2, 128)), vm((nh, nx, out_rows // nx * 3 // 2, 128)),
        vm((ny, nc, per, SHARED)), vm((ny - 1, nc, per, SHARED)),
        vm((nx * nc, rows, SHARED)), vm((nx * nc, rows, SHARED)),
        sems(10), vm((ny * per * width // 128, 128)),
        sems(nx * nc - 1), sems(2, hy * nc * nh), sems(2 * nx - 1), sems(2, n_p), sems(2, n_z), sems(GROUPS, nx - 1), sems(nh * nx - 1), sems(nx - 1), sems(ny - 1), sems(nx * nc - 1),
    ]
    grad_input, grad_weight = pl.pallas_call(
        functools.partial(kernel, dims, scale),
        out_shape=(
            jax.ShapeDtypeStruct((rows, width), bf16),
            jax.ShapeDtypeStruct((cols, out_rows), f32),
        ),
        in_specs=[pl.BlockSpec(memory_space=pltpu.HBM)] * 4,
        out_specs=[pl.BlockSpec(memory_space=pl.ANY)] * 2,
        scratch_shapes=scratch,
        compiler_params=pltpu.CompilerParams(
            collective_id=0, has_side_effects=True, vmem_limit_bytes=40 * 1024 * 1024
        ),
        name="backward",
    )(act_codes, scale_exps, weight, grad_out)
    return grad_input, grad_weight.T


def solution(mesh):
    placed = (P(("ctx", "tp"), None), P(("ctx", "tp"), None), P(None, "tp"), P("ctx", "tp"))
    return jax.shard_map(
        functools.partial(body, DIMS),
        mesh=mesh,
        in_specs=placed,
        out_specs=(P(("ctx", "tp"), None), P("ctx", "tp")),
        check_vma=False,
    )
```

```python
import functools
import math

import jax
import jax.numpy as jnp
from jax import lax
from jax.experimental import pallas as pl
from jax.experimental.pallas import tpu as pltpu
from jax.sharding import PartitionSpec as P

DIMS = {"z": 8, "xh": 2, "core": 2, "xl": 4, "y": 8}
GROUPS = 4
Z_GROUPS = 2
SHARED = 256
FIRST, AFTER_AG1, AFTER_AG2, AFTER_Z1, AFTER_Z2 = 6, 0, 4, 2, 2


def ring_pieces(half, groups):
    low, high = tuple(range(groups // 2)), tuple(range(groups // 2, groups))
    ways = []
    for first, rest in ((low, high), (high, low)):
        order = [(1, g) for g in first]
        for step in range(2, half + 1):
            order += [(step, g) for g in rest + first]
        ways.append(order)
    return ways


def kernel(
    dims, scale, codes_hbm, exps_hbm, w_hbm, g_hbm, gi_out, gw_out,
    gi_ref, gw_ref, out_sem,
    codes, exps, w, wq, wr, g, in_sem,
    s_buf, a1, ab, at, gp, ga, rest, parts, rb, xs, xr, own,
    dwf, dwb, rz, fs, fr, qp, rq, qs, qr,
    gone, filler, s_recv, a_recv, g_recv, p_recv, z_recv, x_recv, f_recv, w_recv, q_recv, o_recv,
):
    nz, nh, nc, nx, ny = dims["z"], dims["xh"], dims["core"], dims["xl"], dims["y"]
    hy, hz = ny // 2, nz // 2
    f32, bf16 = jnp.float32, jnp.bfloat16
    ctx, tp = lax.axis_index("ctx"), lax.axis_index("tp")
    z, xh, c = ctx // (nh * nc), (ctx // nc) % nh, ctx % nc
    xl, y = tp // ny, tp % ny

    def at_z(d):
        return {"ctx": ((z + d + nz) % nz * nh + xh) * nc + c, "tp": tp}

    def at_y(d):
        return {"ctx": ctx, "tp": xl * ny + (y + d + ny) % ny}

    def at_x(dx, dc=0, dh=0):
        return {
            "ctx": (z * nh + (xh + dh) % nh) * nc + (c + dc) % nc,
            "tp": (xl + dx) % nx * ny + y,
        }

    rows, width = codes.shape
    cols, toks = g.shape
    blocks = exps.shape[1]
    quarter = 128 // nx
    feats = width // (nc * nx)
    pfeats = feats // nh
    per = rows * nx
    plain = width - SHARED * nc * nx
    glanes = plain // GROUPS
    sent = {}

    def send(src, dst, kind, rsem, dev):
        copy = pltpu.make_async_remote_copy(
            src_ref=src, dst_ref=dst, send_sem=gone.at[kind], recv_sem=rsem,
            device_id=dev, device_id_type=pl.DeviceIdType.MESH,
        )
        copy.start()
        sent[kind] = sent.get(kind, 0) + math.prod(src.shape)
        return copy

    def wait_all(sem, size):
        same = filler.at[pl.ds(0, size // 128), :]
        pltpu.make_async_copy(same, same, sem).wait()

    loads = []
    moves = [(codes_hbm, codes), (exps_hbm, exps), (g_hbm, g), (w_hbm.at[:, :plain], w)]
    for dx in range(nx):
        first = pl.multiple_of(plain + ((xl + dx) % nx * nc + c) * SHARED, SHARED)
        moves.append((w_hbm.at[:, pl.ds(first, SHARED)], wq.at[dx - 1] if dx else wr.at[xl]))
    for i, (src, dst) in enumerate(moves):
        copy = pltpu.make_async_copy(src, dst, in_sem.at[i])
        copy.start()
        loads.append(copy)

    barrier = pltpu.get_barrier_semaphore()
    mates = [(dx, dc) for dx in range(nx) for dc in range(nc) if (dx, dc) != (0, 0)]
    finals = [(dh, dx) for dh in range(nh)[::-1] for dx in range(nx) if (dh, dx) != (0, 0)]
    peers = [at_x(dx, dc) for dx, dc in mates]
    peers += [at_x(dx, 0, dh) for dh, dx in finals if dh != 0]
    peers += [at_y(d) for d in range(1, ny)]
    peers += [at_z(d) for d in sorted({1, nz - 1, 2 % nz, (nz - 2) % nz} - {0})]
    for dev in peers:
        pl.semaphore_signal(barrier, inc=1, device_id=dev, device_id_type=pl.DeviceIdType.MESH)

    loads[0].wait()
    loads[1].wait()
    scales = jnp.exp2(exps[...].astype(f32))
    lane = lax.broadcasted_iota(jnp.int32, (rows, 128), 1) // quarter
    acts = [
        codes[:, b * 128 : (b + 1) * 128].astype(f32) * scales[:, b : b + 1] for b in range(blocks)
    ]
    for xi in range(nx):
        for ci in range(nc):
            mine = []
            for part in range(nh):
                for zi in range(nz):
                    block = acts[(zi * nh + (part + 1) % nh) * nc + ci]
                    if nh == 2:
                        block = jnp.where(xh == 0, block, acts[(zi * nh + part) * nc + ci])
                    mine.append(block)
            for m in range(len(mine) // nx):
                out = mine[m * nx]
                if xi:
                    out = pltpu.roll(out, (128 - xi * quarter) % 128, 1)
                for i in range(1, nx):
                    piece, shift = mine[m * nx + i], ((i - xi) * quarter) % 128
                    if shift:
                        piece = pltpu.roll(piece, shift, 1)
                    out = jnp.where(lane == i, piece, out)
                s_buf[xi * nc + ci, :, m * 128 : (m + 1) * 128] = out.astype(bf16)
    a1[xl * nc + c] = s_buf[xl * nc + c]

    loads[2].wait()
    raw = g[...].astype(f32).T
    raw = jnp.concatenate(
        [
            raw[(i * ny + j) * rows : (i * ny + j + 1) * rows]
            for j in range(ny) for i in range(nx)
        ],
        axis=0,
    )
    gp[...] = raw.astype(bf16)
    ga[c, xl, :toks, :] = raw[:, :128].astype(bf16)
    tail = raw[:, 128:]
    ga[c, xl, toks:, :] = jnp.concatenate([tail[: toks // 2], tail[toks // 2 :]], axis=1).astype(bf16)

    pl.semaphore_wait(barrier, len(peers))

    s_wait = []
    for k, (dx, dc) in enumerate(mates):
        s_wait.append(
            send(
                s_buf.at[(xl + dx) % nx * nc + (c + dc) % nc], a1.at[xl * nc + c],
                0, s_recv.at[0], at_x(dx, dc),
            )
        )
    g_wait = []
    for dx in range(1, nx):
        g_wait.append(
            send(ga.at[c, xl], ga.at[c, xl], 2, g_recv.at[dx - 1], at_x(dx))
        )
    twin_wait = [
        send(ga.at[c, xl], ga.at[c, xl], 2, g_recv.at[nx - 1], at_x(0, 1))
    ]

    w_wait = []
    for dx in range(nx):
        loads[4 + dx].wait()
        if dx:
            w_wait.append(
                send(wq.at[dx - 1], wr.at[xl], 7, w_recv.at[0], at_x(dx))
            )

    loads[3].wait()
    step_w = min(plain, 512)
    for n in range(plain // step_w):
        part = lax.dot_general(
            gp[...], w[:, n * step_w : (n + 1) * step_w], (((1,), (0,)), ((), ())),
            preferred_element_type=f32,
        )
        parts[:, :, n * step_w : (n + 1) * step_w] = part.astype(bf16).reshape(ny, per, step_w)

    p_orders = ring_pieces(hy, GROUPS)
    p_index = [{piece: i for i, piece in enumerate(order)} for order in p_orders]
    p_copies = [{}, {}]
    p_next = [0, 0]

    def p_piece(way):
        if p_next[way] >= len(p_orders[way]):
            return
        step, grp = p_orders[way][p_next[way]]
        p_next[way] += 1
        sign = 1 - 2 * way
        off = hy + 1 - step
        lanes = slice(grp * glanes, (grp + 1) * glanes)
        dest = (y + sign * off + ny) % ny
        if (step - 1, grp) in p_copies[way]:
            p_copies[way][(step - 1, grp)].wait_recv()
            total = rb[way, step - 2, :, lanes].astype(f32) + parts[dest, :, lanes].astype(f32)
            rb[way, step - 2, :, lanes] = total.astype(bf16)
            src = rb.at[way, step - 2, :, lanes]
        else:
            src = parts.at[dest, :, lanes]
        i = p_index[way][(step, grp)]
        p_copies[way][(step, grp)] = send(
            src, rb.at[way, step - 1, :, lanes], 3, p_recv.at[way, i], at_y(sign)
        )

    def p_both(count=1):
        for _ in range(count):
            p_piece(0)
            p_piece(1)

    p_both(FIRST)

    wait_all(s_recv.at[0], len(mates) * rows * feats)
    for ci in range(nc):
        block = jnp.concatenate([a1[xi * nc + ci].astype(f32) for xi in range(nx)], axis=0).astype(bf16)
        for part in range(nh):
            ab[y, part, ci] = block[:, part * pfeats : (part + 1) * pfeats]

    a_copies = [{}, {}]

    def a_piece(part, way, dist, hops, ci):
        sign = 1 - 2 * way
        ref = ab.at[(y - sign * (dist - hops) + ny) % ny, part, ci]
        i = ((dist - 1) * nc + ci) * nh + part
        a_copies[way][(part, dist, ci)] = send(
            ref, ref, 1, a_recv.at[way, i], at_y(sign * hops)
        )

    def a_all(part, dist, hops):
        for ci in range(nc):
            for way in (0, 1):
                if dist < hy or ci % 2 == way:
                    if dist > 2:
                        a_copies[way][(part, 2, ci)].wait_recv()
                    a_piece(part, way, dist, hops, ci)

    def a_wait(part):
        for way in (0, 1):
            for one, dist, ci in a_copies[way]:
                if one == part and not (dist == 2 and hy > 2):
                    a_copies[way][(one, dist, ci)].wait_recv()

    for part in range(nh):
        if hy > 1:
            a_all(part, 2, 2)
        a_all(part, 1, 1)
    p_both(AFTER_AG1)
    if hy > 2:
        for part in range(nh):
            a_all(part, 3, 1)
            for ci in range(nc):
                a_piece(part, ci % 2, 4, 2, ci)
    p_both(AFTER_AG2)

    for dx in range(1, nx):
        g_wait[dx - 1].wait_recv()
        ref = ga.at[c, (xl - dx + nx) % nx]
        twin_wait.append(
            send(ref, ref, 2, g_recv.at[nx - 1], at_x(0, 1))
        )

    wait_all(g_recv.at[nx - 1], nx * (toks * 3 // 2) * 128)

    mains = nx * 128
    for ci in range(nc):
        for k in range(nx // 2):
            left = ga[ci, 2 * k, toks:, :].astype(f32)
            right = ga[ci, 2 * k + 1, toks:, :].astype(f32)
            first = lax.broadcasted_iota(jnp.int32, left.shape, 1) < 64
            top = jnp.where(first, left, pltpu.roll(right, 64, 1))
            bottom = jnp.where(first, pltpu.roll(left, 64, 1), right)
            lanes = slice(k * 128, (k + 1) * 128)
            rest[ci * toks : ci * toks + toks // 2, lanes] = top.astype(bf16)
            rest[ci * toks + toks // 2 : (ci + 1) * toks, lanes] = bottom.astype(bf16)
    zrows = pfeats // nz

    def dw_part(part):
        feat = slice(part * pfeats, (part + 1) * pfeats)
        for ci in range(nc):
            at[feat, ci * toks : (ci + 1) * toks] = ab[:, part, ci].reshape(toks, pfeats).T

        def store(lanes, value):
            value = value.reshape(nz, zrows, value.shape[1])
            dwf[part, :, :, lanes] = value
            dwb[part, :, :, lanes] = value.astype(bf16)

        for k in range(nx // 2):
            total = None
            for ci in range(nc):
                both = jnp.concatenate([ga[ci, 2 * k, :toks, :], ga[ci, 2 * k + 1, :toks, :]], axis=1)
                some = jnp.dot(at[feat, ci * toks : (ci + 1) * toks], both, preferred_element_type=f32)
                total = some if total is None else total + some
            store(slice(k * 256, (k + 1) * 256), total)
        store(slice(mains, mains + 64 * nx), jnp.dot(at[feat, :], rest[...], preferred_element_type=f32))

    zsub = zrows // Z_GROUPS
    z_copies = [{}, {}]
    halves = [tuple(range(Z_GROUPS // 2)), tuple(range(Z_GROUPS // 2, Z_GROUPS))]

    def z_rows(grp):
        return slice(grp * zsub, (grp + 1) * zsub)

    def z_got(part, way, slot, grp):
        z_copies[way][(part, slot, grp)].wait_recv()
        return rz[way, slot, part, z_rows(grp), :].astype(f32)

    def z_send_piece(part, way, slot, grp, src, hops):
        i = (slot * nh + part) * Z_GROUPS + grp
        z_copies[way][(part, slot, grp)] = send(
            src, rz.at[way, slot, part, z_rows(grp), :], 4, z_recv.at[way, i],
            at_z((1 - 2 * way) * hops),
        )

    def z_round(part, way, slot, off, grp, arrived):
        dest = (z + (1 - 2 * way) * off + nz) % nz
        if not arrived:
            z_send_piece(part, way, slot, grp, dwb.at[part, dest, z_rows(grp), :], 1)
            return
        total = dwf[part, dest, z_rows(grp), :]
        for old in arrived:
            total = total + z_got(part, way, old, grp)
        rz[way, arrived[0], part, z_rows(grp), :] = total.astype(bf16)
        z_send_piece(part, way, slot, grp, rz.at[way, arrived[0], part, z_rows(grp), :], 1)

    def z_each(part, slot, off, has):
        for k in range(Z_GROUPS):
            for way in (0, 1):
                order = halves[1 - way] + halves[way]
                grp = order[k]
                z_round(part, way, slot, off, grp, has(way, grp))

    def z_first(part):
        if hz == 4:
            for k in range(Z_GROUPS // 2):
                for way in (0, 1):
                    grp = halves[way][k]
                    dest = (z + (1 - 2 * way) * 4 + nz) % nz
                    z_send_piece(part, way, 0, grp, dwb.at[part, dest, z_rows(grp), :], 2)
            z_each(part, 1, 3, lambda way, grp: ())
        else:
            for grp in range(Z_GROUPS):
                way = 0 if grp in halves[0] else 1
                z_round(part, way, 0, hz, grp, ())

    for part in range(nh):
        a_wait(part)
        dw_part(part)
        z_first(part)

    wait_all(w_recv.at[0], (nx - 1) * cols * SHARED)
    weights = jnp.concatenate(
        [wr[xi, :128, :] for xi in range(nx)] + [wr[xi, 128:, :] for xi in range(nx)], axis=0
    )
    for ci in range(nc):
        both = jnp.concatenate(
            [ga[ci, xi, :toks, :] for xi in range(nx)] + [rest[ci * toks : (ci + 1) * toks, :]], axis=1
        )
        part = jnp.dot(both, weights, preferred_element_type=f32)
        qp[:, ci] = part.astype(bf16).reshape(ny, per, SHARED)
    q_wait = []
    for near in range(ny // 2, 0, -1):
        for d in sorted({near, ny - near}):
            q_wait.append(
                send(
                    qp.at[(y + d) % ny], rq.at[d - 1], 8, q_recv.at[0], at_y(d)
                )
            )
    p_both(AFTER_Z1)

    if hz == 4:
        for part in range(nh):
            z_each(part, 2, 2, lambda way, grp: (1, 0) if grp in halves[way] else (1,))
        p_both(AFTER_Z2)
        for part in range(nh):
            z_each(part, 3, 1, lambda way, grp: (2,))
    else:
        for step in range(2, hz + 1):
            for part in range(nh):
                z_each(
                    part, step - 1, hz + 1 - step,
                    lambda way, grp: (step - 2,) if step > 2 or grp in halves[way] else (),
                )
    p_both(len(p_orders[0]))

    wait_all(q_recv.at[0], (ny - 1) * nc * per * SHARED)
    for ci in range(nc):
        total = qp[y, ci].astype(f32)
        for d in range(1, ny):
            total = total + rq[d - 1, ci].astype(f32)
        for xi in range(nx):
            qs[xi * nc + ci] = total[xi * rows : (xi + 1) * rows].astype(bf16)
    qr[xl * nc + c] = qs[xl * nc + c]
    o_wait = []
    for k, (dx, dc) in enumerate(mates):
        o_wait.append(
            send(
                qs.at[(xl + dx) % nx * nc + (c + dc) % nc], qr.at[xl * nc + c],
                9, o_recv.at[0], at_x(dx, dc),
            )
        )

    f_wait = []
    for part in range(nh):
        sums = []
        for grp in range(Z_GROUPS):
            total = dwf[part, z, z_rows(grp), :]
            for way in (0, 1):
                if (part, hz - 1, grp) in z_copies[way]:
                    total = total + z_got(part, way, hz - 1, grp)
            sums.append(total)
        total = jnp.concatenate(sums, axis=0)
        half = zrows // 2
        for xi in range(nx):
            fs[part, xi, :zrows, :] = total[:, xi * 128 : (xi + 1) * 128].astype(bf16)
            lo = mains + xi * 64
            last = total[:, lo : lo + 64]
            fs[part, xi, zrows:, :] = jnp.concatenate([last[:half], last[half:]], axis=1).astype(bf16)
        dh = (part + 1) % nh
        if dh == 0:
            fr[xh, xl] = fs[part, xl]
        for k, (far, dx) in enumerate(finals):
            if far == dh:
                f_wait.append(
                    send(
                        fs.at[part, (xl + dx) % nx], fr.at[xh, xl],
                        6, f_recv.at[0], at_x(dx, 0, dh),
                    )
                )

    x_wait = {}
    for grp in p_orders_last(p_orders):
        lanes = slice(grp * glanes, (grp + 1) * glanes)
        total = parts[y, :, lanes].astype(f32)
        for way in (0, 1):
            if (hy, grp) in p_copies[way]:
                p_copies[way][(hy, grp)].wait_recv()
                total = total + rb[way, hy - 1, :, lanes].astype(f32)
        for xi in range(nx):
            piece = total[xi * rows : (xi + 1) * rows]
            own[xi, :, lanes] = piece
            xs[xi, :, lanes] = piece.astype(bf16)
        for dx in range(1, nx):
            x_wait[(grp, dx)] = send(
                xs.at[(xl + dx) % nx, :, lanes], xr.at[dx - 1, :, lanes],
                5, x_recv.at[grp], at_x(dx),
            )

    wait_all(f_recv.at[0], len(finals) * math.prod(fr.shape[2:]))
    firsts, lasts = [], []
    for xi in range(nx):
        total = fr[0, xi].astype(f32)
        for hi in range(1, nh):
            total = total + fr[hi, xi].astype(f32)
        total = total * scale
        height = total.shape[0] * 2 // 3
        firsts.append(total[:height])
        lasts += [total[height:, :64], total[height:, 64:]]
    gw_ref[:128, :] = jnp.concatenate(firsts, axis=0).T
    gw_ref[128:, :] = jnp.concatenate(lasts, axis=0).T
    outs = [pltpu.make_async_copy(gw_ref, gw_out, out_sem.at[0])]
    outs[0].start()

    def put(first, size, i):
        lanes = pl.ds(first, size)
        copy = pltpu.make_async_copy(gi_ref.at[:, lanes], gi_out.at[:, lanes], out_sem.at[i])
        copy.start()
        outs.append(copy)

    wait_all(o_recv.at[0], len(mates) * rows * SHARED)
    for k in range(nx * nc):
        gi_ref[:, plain + k * SHARED : plain + (k + 1) * SHARED] = qr[k]
    put(plain, width - plain, 1)

    for grp in p_orders_last(p_orders):
        lanes = slice(grp * glanes, (grp + 1) * glanes)
        wait_all(x_recv.at[grp], (nx - 1) * rows * glanes)
        total = own[xl, :, lanes]
        for dx in range(1, nx):
            total = total + xr[dx - 1, :, lanes].astype(f32)
        gi_ref[:, lanes] = total.astype(bf16)
        put(grp * glanes, glanes, 2 + grp)

    for kind, size in sent.items():
        wait_all(gone.at[kind], size)
    for copy in outs:
        copy.wait()


def p_orders_last(orders):
    last = orders[0][-1][0]
    return [g for s, g in orders[0] if s == last] if last > 1 else list(range(GROUPS))


def body(dims, act_codes, scale_exps, weight, grad_out):
    weight, grad_out = weight.T, grad_out.T
    act_codes, scale_exps, weight, grad_out = (
        pltpu.with_memory_space_constraint(a, pltpu.HBM) for a in (act_codes, scale_exps, weight, grad_out)
    )
    nz, nh, nc, nx, ny = dims["z"], dims["xh"], dims["core"], dims["xl"], dims["y"]
    hy, hz = ny // 2, nz // 2
    rows, width = act_codes.shape
    cols, toks = grad_out.shape
    out_rows = width // (nz * nh * nc)
    feats = width // (nc * nx)
    per = rows * nx
    dcols = nx * cols
    scale = float(1.0 / (toks * nz * nh * nc) ** 0.5)
    bf16, f32 = jnp.bfloat16, jnp.float32
    n_p = GROUPS // 2 + (hy - 1) * GROUPS
    n_z = hz * nh * Z_GROUPS
    plain = width - SHARED * nc * nx

    def vm(shape, kind=bf16):
        return pltpu.VMEM(shape, kind)

    def sems(*shape):
        return pltpu.SemaphoreType.DMA(shape)

    scratch = [
        vm(act_codes.shape), vm((cols, out_rows), f32), sems(2 + GROUPS),
        vm(act_codes.shape), vm(scale_exps.shape, jnp.int32), vm((cols, plain)),
        vm((nx - 1, cols, SHARED)), vm((nx, cols, SHARED)), vm(grad_out.shape), sems(4 + nx),
        vm((nx * nc, rows, feats)), vm((nx * nc, rows, feats)), vm((ny, nh, nc, per, feats // nh)),
        vm((feats, nc * toks)), vm((toks, cols)), vm((nc, nx, toks * 3 // 2, 128)),
        vm((nc * toks, 64 * nx)), vm((ny, per, plain)), vm((2, hy, per, plain)),
        vm((nx, rows, plain)), vm((nx - 1, rows, plain)), vm((nx, rows, plain), f32),
        vm((nh, nz, feats // nh // nz, dcols), f32), vm((nh, nz, feats // nh // nz, dcols)),
        vm((2, hz, nh, feats // nh // nz, dcols)),
        vm((nh, nx, out_rows // nx * 3 // 2, 128)), vm((nh, nx, out_rows // nx * 3 // 2, 128)),
        vm((ny, nc, per, SHARED)), vm((ny - 1, nc, per, SHARED)),
        vm((nx * nc, rows, SHARED)), vm((nx * nc, rows, SHARED)),
        sems(10), vm((ny * per * width // 128, 128)),
        sems(1), sems(2, hy * nc * nh), sems(nx), sems(2, n_p), sems(2, n_z), sems(GROUPS), sems(1), sems(1), sems(1), sems(1),
    ]
    grad_input, grad_weight = pl.pallas_call(
        functools.partial(kernel, dims, scale),
        out_shape=(
            jax.ShapeDtypeStruct((rows, width), bf16),
            jax.ShapeDtypeStruct((cols, out_rows), f32),
        ),
        in_specs=[pl.BlockSpec(memory_space=pltpu.HBM)] * 4,
        out_specs=[pl.BlockSpec(memory_space=pl.ANY)] * 2,
        scratch_shapes=scratch,
        compiler_params=pltpu.CompilerParams(
            collective_id=0, has_side_effects=True, vmem_limit_bytes=40 * 1024 * 1024
        ),
        name="backward",
    )(act_codes, scale_exps, weight, grad_out)
    return grad_input, grad_weight.T


def solution(mesh):
    placed = (P(("ctx", "tp"), None), P(("ctx", "tp"), None), P(None, "tp"), P("ctx", "tp"))
    return jax.shard_map(
        functools.partial(body, DIMS),
        mesh=mesh,
        in_specs=placed,
        out_specs=(P(("ctx", "tp"), None), P("ctx", "tp")),
        check_vma=False,
    )
```
